16 devices in a mesh: data: 2 (over y, z), ctx: 8 (over x, core).
Axes of the slice: x: 4, y: 2, z: 1, core: 2. Of those that a mesh axis runs over, the one named last changes fastest.
The devices are a block of a 4x4x8 slice.
Arguments:
- hidden: bfloat16 [512, 4096], P(('data', 'ctx')), parts along dimension 0
- seq_lens: int32 [512], P(('data', 'ctx')), parts along dimension 0
- w_query: bfloat16 [4, 4096, 4096], replicated
- w_key: bfloat16 [4, 4096, 1024], replicated
- w_value: bfloat16 [4, 4096, 1024], replicated
- w_out: bfloat16 [4, 4096, 4096], replicated
- k_prefix: bfloat16 [4, 8192, 8, 128], P(None, ('data', 'ctx')), parts along dimension 1
- v_prefix: bfloat16 [4, 8192, 8, 128], P(None, ('data', 'ctx')), parts along dimension 1
- k_suffix: bfloat16 [4, 512, 32, 8, 128], P(None, ('data', 'ctx')), parts along dimension 1
- v_suffix: bfloat16 [4, 512, 32, 8, 128], P(None, ('data', 'ctx')), parts along dimension 1
Outputs:
- output 1: bfloat16 [512, 4096], P(('data', 'ctx')), parts along dimension 0
- output 2: bfloat16 [4, 512, 32, 8, 128], P(None, ('data', 'ctx')), parts along dimension 1
- output 3: bfloat16 [4, 512, 32, 8, 128], P(None, ('data', 'ctx')), parts along dimension 1
There are 2 independent parts. The reference program is written for one: setup_inputs(seed, part) draws one part's arguments, and reference() takes and returns one part's arrays. A program takes and returns all parts, laid end to end along the dimension named above; an argument that names none is the same for every part.
All inputs are finite; a program needn't handle non-finite values.
Results may differ from the reference program's by a relative error of at most 0.0139564.
Values are sent between devices in bfloat16 or wider.
A program may use at most 768 MiB of HBM per device.

```python
import jax
import jax.numpy as jnp
from jax import lax

MODEL_DIM = 4096
NUM_HEADS = 32
KV_HEADS = 8
HEAD_DIM = 128
LAYERS = 4
SHARDS = 8
BATCH_SIZE = 256
PREFIX_LEN = 4096
SUFFIX_LEN = 32
HOME_ROWS = 32


def setup_inputs(seed: int = 0, part: int = 0) -> dict:
    shared_keys = jax.random.split(jax.random.key(seed), 4)
    part_keys = jax.random.split(jax.random.fold_in(jax.random.key(seed + 1), part), 10)
    q_width = NUM_HEADS * HEAD_DIM
    kv_width = KV_HEADS * HEAD_DIM
    shard_rows = PREFIX_LEN // SHARDS
    w_query = jax.random.normal(shared_keys[0], (LAYERS, MODEL_DIM, q_width), jnp.float32) * MODEL_DIM ** -0.5
    w_key = jax.random.normal(shared_keys[1], (LAYERS, MODEL_DIM, kv_width), jnp.float32) * (2.5 * MODEL_DIM ** -0.5)
    w_value = jax.random.normal(shared_keys[2], (LAYERS, MODEL_DIM, kv_width), jnp.float32) * MODEL_DIM ** -0.5
    w_out = jax.random.normal(shared_keys[3], (LAYERS, q_width, MODEL_DIM), jnp.float32) * (q_width * LAYERS) ** -0.5
    hidden = jax.random.normal(part_keys[0], (BATCH_SIZE, MODEL_DIM), jnp.float32)
    centre_shape = (LAYERS, SHARDS, 1, KV_HEADS, HEAD_DIM)
    block_shape = (LAYERS, SHARDS, shard_rows, KV_HEADS, HEAD_DIM)
    prefix_shape = (LAYERS, PREFIX_LEN, KV_HEADS, HEAD_DIM)
    k_prefix = (1.5 * jax.random.normal(part_keys[1], centre_shape, jnp.float32) + jax.random.normal(part_keys[2], block_shape, jnp.float32)).reshape(prefix_shape)
    v_prefix = (jax.random.normal(part_keys[3], centre_shape, jnp.float32) + 0.5 * jax.random.normal(part_keys[4], block_shape, jnp.float32)).reshape(prefix_shape)
    seq_centre = (LAYERS, BATCH_SIZE, 1, KV_HEADS, HEAD_DIM)
    suffix_shape = (LAYERS, BATCH_SIZE, SUFFIX_LEN, KV_HEADS, HEAD_DIM)
    k_suffix = 2.5 * jax.random.normal(part_keys[5], seq_centre, jnp.float32) + jax.random.normal(part_keys[6], suffix_shape, jnp.float32)
    v_suffix = jax.random.normal(part_keys[7], seq_centre, jnp.float32) + 0.5 * jax.random.normal(part_keys[8], suffix_shape, jnp.float32)
    len_keys = jax.random.split(part_keys[9], 2)
    seq_lens = jax.random.randint(len_keys[0], (BATCH_SIZE,), 0, SUFFIX_LEN, dtype=jnp.int32)
    longest = jax.random.randint(len_keys[1], (), 0, BATCH_SIZE, dtype=jnp.int32)
    seq_lens = seq_lens.at[longest].set(SUFFIX_LEN - 1)
    seq_lens = seq_lens.at[(longest + BATCH_SIZE // 2) % BATCH_SIZE].set(0)
    return {'hidden': hidden.astype(jnp.bfloat16), 'seq_lens': seq_lens, 'w_query': w_query.astype(jnp.bfloat16), 'w_key': w_key.astype(jnp.bfloat16), 'w_value': w_value.astype(jnp.bfloat16), 'w_out': w_out.astype(jnp.bfloat16), 'k_prefix': k_prefix.astype(jnp.bfloat16), 'v_prefix': v_prefix.astype(jnp.bfloat16), 'k_suffix': k_suffix.astype(jnp.bfloat16), 'v_suffix': v_suffix.astype(jnp.bfloat16)}


def attend_block(queries, k_pre, v_pre, k_suf, v_suf, slot_live):
    score_scale = HEAD_DIM ** -0.5
    pre_scores = jnp.einsum('bkgd,pkd->bkgp', queries, k_pre) * score_scale
    suf_scores = jnp.einsum('bkgd,bskd->bkgs', queries, k_suf) * score_scale
    suf_scores = jnp.where(slot_live[:, None, None, :], suf_scores, -jnp.inf)
    row_max = jnp.maximum(pre_scores.max(axis=-1), suf_scores.max(axis=-1))
    pre_exp = jnp.exp(pre_scores - row_max[..., None])
    suf_exp = jnp.exp(suf_scores - row_max[..., None])
    mass_sum = pre_exp.sum(axis=-1) + suf_exp.sum(axis=-1)
    mixed_sum = jnp.einsum('bkgp,pkd->bkgd', pre_exp, v_pre) + jnp.einsum('bkgs,bskd->bkgd', suf_exp, v_suf)
    return mixed_sum / mass_sum[..., None]


def reference(hidden, seq_lens, w_query, w_key, w_value, w_out, k_prefix, v_prefix, k_suffix, v_suffix):
    group_size = NUM_HEADS // KV_HEADS
    blocks = BATCH_SIZE // HOME_ROWS
    slot_ids = jnp.arange(SUFFIX_LEN, dtype=jnp.int32)[None, :]
    slot_hit = (slot_ids == seq_lens[:, None])[:, :, None, None]
    slot_live = slot_ids <= seq_lens[:, None]
    live_blocks = slot_live.reshape(blocks, HOME_ROWS, SUFFIX_LEN)

    def layer_step(hidden_state, layer_args):
        q_weight, k_weight, v_weight, o_weight, k_pre, v_pre, k_suf, v_suf = layer_args
        queries = jnp.dot(hidden_state, q_weight, preferred_element_type=jnp.float32).astype(jnp.bfloat16)
        k_new = jnp.dot(hidden_state, k_weight, preferred_element_type=jnp.float32).astype(jnp.bfloat16).reshape(BATCH_SIZE, 1, KV_HEADS, HEAD_DIM)
        v_new = jnp.dot(hidden_state, v_weight, preferred_element_type=jnp.float32).astype(jnp.bfloat16).reshape(BATCH_SIZE, 1, KV_HEADS, HEAD_DIM)
        k_suf = jnp.where(slot_hit, k_new, k_suf)
        v_suf = jnp.where(slot_hit, v_new, v_suf)
        q_blocks = queries.astype(jnp.float32).reshape(blocks, HOME_ROWS, KV_HEADS, group_size, HEAD_DIM)
        k_full = k_pre.astype(jnp.float32)
        v_full = v_pre.astype(jnp.float32)
        k_blocks = k_suf.astype(jnp.float32).reshape(blocks, HOME_ROWS, SUFFIX_LEN, KV_HEADS, HEAD_DIM)
        v_blocks = v_suf.astype(jnp.float32).reshape(blocks, HOME_ROWS, SUFFIX_LEN, KV_HEADS, HEAD_DIM)
        attended = lax.map(lambda block_args: attend_block(block_args[0], k_full, v_full, block_args[1], block_args[2], block_args[3]), (q_blocks, k_blocks, v_blocks, live_blocks))
        attended = attended.astype(jnp.bfloat16).reshape(BATCH_SIZE, NUM_HEADS * HEAD_DIM)
        update = jnp.dot(attended, o_weight, preferred_element_type=jnp.float32).astype(jnp.bfloat16)
        hidden_state = (hidden_state.astype(jnp.float32) + update.astype(jnp.float32)).astype(jnp.bfloat16)
        return hidden_state, (k_suf, v_suf)

    hidden_out, cache_out = lax.scan(layer_step, hidden, (w_query, w_key, w_value, w_out, k_prefix, v_prefix, k_suffix, v_suffix))
    return hidden_out, cache_out[0], cache_out[1]
```

```python
import functools
import math

import jax
import jax.numpy as jnp
from jax import lax
from jax.experimental import pallas as pl
from jax.experimental.pallas import tpu as pltpu
from jax.sharding import PartitionSpec as P

MESH = pl.DeviceIdType.MESH
F32 = jnp.float32
BF16 = jnp.bfloat16
NEG = -1e30


def decode_kernel(cfg, lens_ref, hid_ref, wq, wk, wv, wo, kp, vp, ks, vs,
                  out_ref, kn_ref, vn_ref,
                  wbuf, xbuf, qkv, qx, qall, raw, kf, kvsrc, kvbuf, sfx, sscr, osend, lsend, orecv, lrecv,
                  q3, n3, o3, l3, obuf,
                  w_sem, raw_sem, sfx_sem, x0_sem, q_ssem, q_rsem, qx_sem, kv_ssem, kv_rsem,
                  o_ssem, o_rsem, l_ssem, l_rsem, ob_sem, x_ssem, x_rsem):
    n_ctx, layers, rows, dim, kvh, grp, hd, pos, slots, nslot, ch = cfg
    chips = n_ctx // 2
    qw = grp * hd
    half_q = chips * qw
    half_kv = chips * hd
    xw = dim // (2 * chips)
    steps = 2 * chips + 2
    total = layers * steps
    scale = hd ** -0.5
    me = lax.axis_index('ctx')
    p = me // 2
    c = me % 2
    mate = 2 * p + (1 - c)
    my_head = chips * c + p
    my_rows = pl.ds(pl.multiple_of(c * rows, rows), rows)
    mate_rows = pl.ds(pl.multiple_of((1 - c) * rows, rows), rows)

    def owner_at(t):
        return (p + lax.rem(t + chips // 2, chips)) % chips if not isinstance(t, int) else (p + (t + chips // 2) % chips) % chips

    def issue_weights(g):
        lyr = g // steps
        j = g % steps
        slot = g % nslot

        @pl.when(g < total)
        def _():
            @pl.when(j < chips)
            def _():
                dest = (p + (j + chips // 2) % chips) % chips
                off = pl.multiple_of(c * half_q + dest * qw, 128)
                pltpu.make_async_copy(wq.at[lyr, :, pl.ds(off, qw)], wbuf.at[slot], w_sem.at[slot]).start()

            @pl.when(j == chips)
            def _():
                off = pl.multiple_of(c * half_kv, 128)
                pltpu.make_async_copy(wk.at[lyr, :, pl.ds(off, half_kv)], wbuf.at[slot], w_sem.at[slot]).start()

            @pl.when(j == chips + 1)
            def _():
                off = pl.multiple_of(c * half_kv, 128)
                pltpu.make_async_copy(wv.at[lyr, :, pl.ds(off, half_kv)], wbuf.at[slot], w_sem.at[slot]).start()

            @pl.when(j > chips + 1)
            def _():
                off = pl.multiple_of(c * (dim // 2) + (j - chips - 2) * xw, 128)
                pltpu.make_async_copy(wo.at[lyr, :, pl.ds(off, xw)], wbuf.at[slot], w_sem.at[slot]).start()

    def wait_weights(g):
        slot = g % nslot
        pltpu.make_async_copy(wq.at[0, :, pl.ds(0, qw)], wbuf.at[slot], w_sem.at[slot]).wait()
        return slot

    def raw_copies(lyr):
        return (pltpu.make_async_copy(kp.at[lyr], raw.at[0], raw_sem.at[0]),
                pltpu.make_async_copy(vp.at[lyr], raw.at[1], raw_sem.at[1]))

    def wait_kv_sent(slot):
        for t in range(2):
            full = kvsrc.at[slot, t, pl.ds(0, n_ctx - 1)]
            pltpu.make_async_remote_copy(full, full, kv_ssem.at[slot, t], kv_rsem.at[0, 0],
                                         device_id={'ctx': mate}, device_id_type=MESH).wait_send()

    def prep_kv(lyr):
        slot = lyr % 2
        for cp in raw_copies(lyr):
            cp.wait()
        blk = 64
        for t in range(2):
            def step(r, _):
                kf[...] = raw[t, pl.ds(pl.multiple_of(r * blk * kvh, 16), blk * kvh), :].astype(F32)
                for h in range(kvh):
                    kvsrc[slot, t, h, pl.ds(pl.multiple_of(r * blk, blk), blk), :] = kf[pl.ds(h, blk, stride=kvh), :].astype(BF16)
                return 0
            lax.fori_loop(0, pos // blk, step, 0)
            kvbuf[lyr, t, pl.ds(pl.multiple_of(me * pos, pos), pos), :] = kvsrc[slot, t, my_head]

        @pl.when(lyr + 1 < layers)
        def _():
            for cp in raw_copies(lyr + 1):
                cp.start()

    def send_kv(lyr):
        slot = lyr % 2
        for j in range(1, n_ctx):
            dest = (me + j) % n_ctx
            head = chips * (dest % 2) + dest // 2
            for t in range(2):
                pltpu.make_async_remote_copy(
                    kvsrc.at[slot, t, head], kvbuf.at[lyr, t, pl.ds(pl.multiple_of(me * pos, pos), pos)],
                    kv_ssem.at[slot, t], kv_rsem.at[lyr, t], device_id={'ctx': dest}, device_id_type=MESH).start()

    def wait_kv(lyr):
        for t in range(2):
            part = kvbuf.at[lyr, t, pl.ds(0, (n_ctx - 1) * pos)]
            pltpu.make_async_remote_copy(part, part, kv_ssem.at[0, 0], kv_rsem.at[lyr, t],
                                         device_id={'ctx': mate}, device_id_type=MESH).wait_recv()

    def sfx_copies(lyr):
        return (pltpu.make_async_copy(ks.at[lyr], sfx.at[0], sfx_sem.at[0]),
                pltpu.make_async_copy(vs.at[lyr], sfx.at[1], sfx_sem.at[1]))

    for cp in raw_copies(0):
        cp.start()
    for g in range(nslot):
        issue_weights(jnp.int32(g))
    for cp in sfx_copies(0):
        cp.start()
    barrier = pltpu.get_barrier_semaphore()
    for j in range(1, n_ctx):
        pl.semaphore_signal(barrier, inc=1, device_id={'ctx': (me + j) % n_ctx}, device_id_type=MESH)
    xbuf[0, my_rows, :] = hid_ref[...]
    pl.semaphore_wait(barrier, n_ctx - 1)
    x0 = pltpu.make_async_remote_copy(xbuf.at[0, my_rows], xbuf.at[0, my_rows], x0_sem.at[0], x0_sem.at[1],
                                      device_id={'ctx': mate}, device_id_type=MESH)
    x0.start()
    prep_kv(jnp.int32(0))
    send_kv(jnp.int32(0))
    x0.wait()

    def q_copy(dest):
        return pltpu.make_async_remote_copy(qkv.at[dest], qall.at[p], q_ssem.at[dest], q_rsem.at[p],
                                            device_id={'ctx': 2 * dest + c}, device_id_type=MESH)

    def q_recv(src):
        return pltpu.make_async_remote_copy(qkv.at[src], qall.at[src], q_ssem.at[src], q_rsem.at[src],
                                            device_id={'ctx': mate}, device_id_type=MESH)

    def o_copy(dest, cc):
        return pltpu.make_async_remote_copy(osend.at[dest, cc], orecv.at[my_head], o_ssem.at[dest, cc], o_rsem.at[my_head],
                                            device_id={'ctx': 2 * dest + cc}, device_id_type=MESH)

    def l_copy(dest, cc):
        return pltpu.make_async_remote_copy(lsend.at[dest, cc], lrecv.at[my_head], l_ssem.at[dest, cc], l_rsem.at[my_head],
                                            device_id={'ctx': 2 * dest + cc}, device_id_type=MESH)

    def layer(lyr, _):
        cur = lyr % 2
        nxt = 1 - cur
        base = lyr * steps

        def proj(t, _):
            g = base + t
            slot = wait_weights(g)
            val = jnp.dot(xbuf[cur], wbuf[slot], preferred_element_type=F32).astype(BF16)
            dest = jnp.where(t < chips, (p + (t + chips // 2) % chips) % chips, t)
            qkv[dest] = val

            @pl.when(t < chips)
            def _():
                @pl.when(dest != p)
                def _():
                    q_copy(dest).start()

                @pl.when(dest == p)
                def _():
                    qall[p] = val
            issue_weights(g + nslot)
            return 0

        lax.fori_loop(0, chips + 2, proj, 0)
        qx_cp = pltpu.make_async_remote_copy(qkv.at[:, mate_rows], qx, qx_sem.at[0], qx_sem.at[1],
                                             device_id={'ctx': mate}, device_id_type=MESH)
        qx_cp.start()

        @pl.when(lyr + 1 < layers)
        def _():
            @pl.when(lyr >= 1)
            def _():
                wait_kv_sent((lyr + 1) % 2)
            prep_kv(lyr + 1)

        wait_kv(lyr)

        def attend(t, _):
            src = (p + (t + 1) % chips) % chips

            @pl.when(src != p)
            def _():
                q_recv(src).wait_recv()
            qv = jnp.concatenate([qall[src, cc * rows:(cc + 1) * rows, g * hd:(g + 1) * hd]
                                  for cc in range(2) for g in range(grp)], axis=0)
            n_rows = 2 * grp * rows
            mx = jnp.full((n_rows, hd), NEG, F32)
            for j in range(n_ctx * pos // ch):
                s = lax.dot_general(qv, kvbuf[lyr, 0, j * ch:(j + 1) * ch, :], (((1,), (1,)), ((), ())), preferred_element_type=F32)
                sscr[:, j * ch:(j + 1) * ch] = s
                for b in range(ch // hd):
                    mx = jnp.maximum(mx, s[:, b * hd:(b + 1) * hd])
            m = mx.max(axis=-1, keepdims=True)
            acc = jnp.zeros((n_rows, hd), F32)
            ls = jnp.zeros((n_rows, hd), F32)
            for j in range(n_ctx * pos // ch):
                e = jnp.exp((sscr[:, j * ch:(j + 1) * ch] - m) * scale)
                for b in range(ch // hd):
                    ls = ls + e[:, b * hd:(b + 1) * hd]
                acc = acc + jnp.dot(e.astype(BF16), kvbuf[lyr, 1, j * ch:(j + 1) * ch, :], preferred_element_type=F32)
            mass = ls.sum(axis=-1, keepdims=True)
            o = (acc / mass).astype(BF16)
            lse = jnp.broadcast_to(m * scale + jnp.log(mass), (n_rows, hd))
            per = grp * rows
            for cc in range(2):
                dev = 2 * src + cc
                for g in range(grp):
                    osend[src, cc, :, g * hd:(g + 1) * hd] = o[cc * per + g * rows: cc * per + (g + 1) * rows]
                lsend[src, cc] = jnp.transpose(lse[cc * per:(cc + 1) * per])[0:8]

                @pl.when(dev != me)
                def _():
                    o_copy(src, cc).start()
                    l_copy(src, cc).start()

                @pl.when(dev == me)
                def _():
                    orecv[my_head] = osend[src, cc]
                    lrecv[my_head] = lsend[src, cc]
            return 0

        lax.fori_loop(0, chips, attend, 0)

        @pl.when(lyr + 1 < layers)
        def _():
            send_kv(lyr + 1)

        qx_cp.wait_recv()
        mine = c * 1
        for h in range(kvh):
            own = mine == h // chips
            hh = h % chips
            for g in range(grp):
                sel = jnp.where(own, qkv[hh, my_rows, g * hd:(g + 1) * hd].astype(F32), qx[hh, :, g * hd:(g + 1) * hd].astype(F32))
                q3[pl.ds(h * grp + g, rows, stride=kvh * grp), :] = sel
            for t in range(2):
                sel = jnp.where(own, qkv[chips + t, my_rows, hh * hd:(hh + 1) * hd].astype(F32), qx[chips + t, :, hh * hd:(hh + 1) * hd].astype(F32))
                n3[t, pl.ds(h, rows, stride=kvh), :] = sel
                (kn_ref, vn_ref)[t][lyr, :, h * hd:(h + 1) * hd] = sel.astype(BF16)
        for cp in sfx_copies(lyr):
            cp.wait()
        nh = kvh * grp
        cols = slots * kvh
        row_slot = lax.broadcasted_iota(jnp.int32, (cols, hd), 0) // kvh
        col_id = lax.broadcasted_iota(jnp.int32, (nh, cols), 1)
        row_id = lax.broadcasted_iota(jnp.int32, (nh, cols), 0)
        same = (col_id % kvh) == (row_id // grp)
        col_slot = jnp.where(same, col_id // kvh, slots + 1)
        unroll = 4

        def suffix(i, _):
            for u in range(unroll):
                b = i * unroll + u
                ln = lens_ref[b]
                hit = row_slot == ln
                kv = []
                for t in range(2):
                    new = n3[t, pl.ds(pl.multiple_of(b * kvh, kvh), kvh), :]
                    new = jnp.broadcast_to(new[None], (slots, kvh, hd)).reshape(cols, hd)
                    kv.append(jnp.where(hit, new, sfx[t, b].astype(F32)).astype(BF16))
                at = pl.ds(pl.multiple_of(b * nh, nh), nh)
                s = lax.dot_general(q3[at, :].astype(BF16), kv[0], (((1,), (1,)), ((), ())), preferred_element_type=F32) * scale
                s = jnp.where(col_slot <= ln, s, -jnp.inf)
                m = s.max(axis=-1, keepdims=True)
                e = jnp.exp(s - m)
                mass = e.sum(axis=-1, keepdims=True)
                o3[at, :] = jnp.dot(e.astype(BF16), kv[1], preferred_element_type=F32) / mass
                l3[at, :] = jnp.broadcast_to(m + jnp.log(mass), (nh, hd))
            return 0

        lax.fori_loop(0, rows // unroll, suffix, 0)

        @pl.when(lyr + 1 < layers)
        def _():
            for cp in sfx_copies(lyr + 1):
                cp.start()

        for h in range(kvh):
            @pl.when(my_head != h)
            def _():
                pltpu.make_async_remote_copy(osend.at[0, 0], orecv.at[h], o_ssem.at[0, 0], o_rsem.at[h],
                                             device_id={'ctx': mate}, device_id_type=MESH).wait_recv()
                pltpu.make_async_remote_copy(lsend.at[0, 0], lrecv.at[h], l_ssem.at[0, 0], l_rsem.at[h],
                                             device_id={'ctx': mate}, device_id_type=MESH).wait_recv()
            lp = jnp.transpose(jnp.concatenate([lrecv[h]] * (hd // 8), axis=0))
            for g in range(grp):
                lpg = lp[g * rows:(g + 1) * rows]
                hx = h * grp + g
                ls = l3[pl.ds(hx, rows, stride=kvh * grp), :]
                os = o3[pl.ds(hx, rows, stride=kvh * grp), :]
                top = jnp.maximum(lpg, ls)
                wp = jnp.exp(lpg - top)
                ws = jnp.exp(ls - top)
                mix = (wp * orecv[h, :, g * hd:(g + 1) * hd].astype(F32) + ws * os) / (wp + ws)
                obuf[my_rows, hx * hd:(hx + 1) * hd] = mix.astype(BF16)
        ob = pltpu.make_async_remote_copy(obuf.at[my_rows], obuf.at[my_rows], ob_sem.at[0], ob_sem.at[1],
                                          device_id={'ctx': mate}, device_id_type=MESH)
        ob.start()
        ob.wait_recv()

        def x_copy(n):
            col = pl.ds(pl.multiple_of(c * (dim // 2) + n * xw, 128), xw)
            return pltpu.make_async_remote_copy(xbuf.at[nxt, :, col], xbuf.at[nxt, :, col], x_ssem.at[n], x_rsem.at[n],
                                                device_id={'ctx': mate}, device_id_type=MESH)

        def outp(n, _):
            g = base + chips + 2 + n
            slot = wait_weights(g)
            upd = jnp.dot(obuf[...], wbuf[slot], preferred_element_type=F32).astype(BF16)
            col = pl.ds(pl.multiple_of(c * (dim // 2) + n * xw, 128), xw)
            xbuf[nxt, :, col] = (xbuf[cur, :, col].astype(F32) + upd.astype(F32)).astype(BF16)
            x_copy(n).start()
            issue_weights(g + nslot)
            return 0

        lax.fori_loop(0, chips, outp, 0)

        qx_cp.wait_send()
        ob.wait_send()
        for t in range(chips):
            @pl.when(p != t)
            def _():
                q_copy(jnp.int32(t)).wait_send()
            for cc in range(2):
                @pl.when(me != 2 * t + cc)
                def _():
                    o_copy(t, cc).wait_send()
                    l_copy(t, cc).wait_send()
        for n in range(chips):
            x_copy(n).wait()
        return 0

    lax.fori_loop(0, layers, layer, 0)
    for back in range(min(2, layers)):
        wait_kv_sent((layers - 1 - back) % 2)
    out_ref[...] = xbuf[layers % 2, my_rows, :]


def solution(mesh):
    n_ctx = mesh.shape['ctx']
    home_axes = ('data', 'ctx')
    row_spec = P(home_axes, None)
    lens_spec = P(home_axes)
    whole_spec = P()
    prefix_spec = P(None, home_axes, None, None)
    cache_spec = P(None, home_axes, None, None, None)

    def local_step(hidden, seq_lens, w_query, w_key, w_value, w_out, k_prefix, v_prefix, k_suffix, v_suffix):
        layers, pos, kvh, hd = k_prefix.shape
        rows, dim = hidden.shape
        slots = k_suffix.shape[2]
        grp = w_query.shape[2] // (kvh * hd)
        chips = n_ctx // 2
        qw = grp * hd
        nslot = 7
        ch = min(1024, n_ctx * pos)
        cfg = (n_ctx, layers, rows, dim, kvh, grp, hd, pos, slots, nslot, ch)
        assert kvh == n_ctx and chips * hd == qw and dim // n_ctx == qw and grp * rows == hd
        nh = kvh * grp
        vmem, anys, smem = pltpu.VMEM, pl.ANY, pltpu.SMEM
        hidden_out, k_new, v_new = pl.pallas_call(
            functools.partial(decode_kernel, cfg),
            out_shape=(jax.ShapeDtypeStruct((rows, dim), BF16),
                       jax.ShapeDtypeStruct((layers, rows, kvh * hd), BF16),
                       jax.ShapeDtypeStruct((layers, rows, kvh * hd), BF16)),
            in_specs=[pl.BlockSpec(memory_space=smem), pl.BlockSpec(memory_space=vmem)] + [pl.BlockSpec(memory_space=anys)] * 8,
            out_specs=[pl.BlockSpec(memory_space=vmem)] * 3,
            scratch_shapes=[
                vmem((nslot, dim, qw), BF16),
                vmem((2, 2 * rows, dim), BF16),
                vmem((chips + 2, 2 * rows, qw), BF16),
                vmem((chips + 2, rows, qw), BF16),
                vmem((chips, 2 * rows, qw), BF16),
                vmem((2, pos * kvh, hd), BF16),
                vmem((64 * kvh, hd), F32),
                vmem((2, 2, kvh, pos, hd), BF16),
                vmem((layers, 2, n_ctx * pos, hd), BF16),
                vmem((2, rows, slots * kvh, hd), BF16),
                vmem((2 * grp * rows, n_ctx * pos), F32),
                vmem((chips, 2, rows, qw), BF16),
                vmem((chips, 2, 8, hd), F32),
                vmem((kvh, rows, qw), BF16),
                vmem((kvh, 8, hd), F32),
                vmem((rows * nh, hd), F32),
                vmem((2, rows * kvh, hd), F32),
                vmem((rows * nh, hd), F32),
                vmem((rows * nh, hd), F32),
                vmem((2 * rows, nh * hd), BF16),
                pltpu.SemaphoreType.DMA((nslot,)),
                pltpu.SemaphoreType.DMA((2,)),
                pltpu.SemaphoreType.DMA((2,)),
                pltpu.SemaphoreType.DMA((2,)),
                pltpu.SemaphoreType.DMA((chips,)),
                pltpu.SemaphoreType.DMA((chips,)),
                pltpu.SemaphoreType.DMA((2,)),
                pltpu.SemaphoreType.DMA((2, 2)),
                pltpu.SemaphoreType.DMA((layers, 2)),
                pltpu.SemaphoreType.DMA((chips, 2)),
                pltpu.SemaphoreType.DMA((kvh,)),
                pltpu.SemaphoreType.DMA((chips, 2)),
                pltpu.SemaphoreType.DMA((kvh,)),
                pltpu.SemaphoreType.DMA((2,)),
                pltpu.SemaphoreType.DMA((chips,)),
                pltpu.SemaphoreType.DMA((chips,)),
            ],
            compiler_params=pltpu.CompilerParams(collective_id=0, has_side_effects=True, vmem_limit_bytes=67043328),
            name='decode_layers',
        )(seq_lens, hidden, w_query, w_key, w_value, w_out,
          k_prefix.reshape(layers, pos * kvh, hd), v_prefix.reshape(layers, pos * kvh, hd),
          k_suffix.reshape(layers, rows, slots * kvh, hd), v_suffix.reshape(layers, rows, slots * kvh, hd))
        hit = (lax.broadcasted_iota(jnp.int32, (rows, slots), 1) == seq_lens[:, None])[None, :, :, None, None]
        k_out = jnp.where(hit, k_new.reshape(layers, rows, 1, kvh, hd), k_suffix)
        v_out = jnp.where(hit, v_new.reshape(layers, rows, 1, kvh, hd), v_suffix)
        return hidden_out, k_out, v_out

    return jax.shard_map(local_step, mesh=mesh, in_specs=(row_spec, lens_spec, whole_spec, whole_spec, whole_spec, whole_spec, prefix_spec, prefix_spec, cache_spec, cache_spec), out_specs=(row_spec, cache_spec, cache_spec), check_vma=False)
```

```python
import functools
import math

import jax
import jax.numpy as jnp
from jax import lax
from jax.experimental import pallas as pl
from jax.experimental.pallas import tpu as pltpu
from jax.sharding import PartitionSpec as P

MESH = pl.DeviceIdType.MESH
F32 = jnp.float32
BF16 = jnp.bfloat16
NEG = -1e30
UNROLL = 8
EARLY = 2
PACED = False
LOG2E = 1.4426950408889634


def decode_kernel(cfg, lens_ref, hid_ref, wq, wk, wv, wo, kp, vp, ks, vs,
                  out_ref, kn_ref, vn_ref,
                  wbuf, xbuf, qkv, qx, qall, raw, kf, kvsrc, kvbuf, sfx, sscr, osend, lsend, orecv, lrecv,
                  q3, n3, o3, l3, obuf,
                  w_sem, raw_sem, sfx_sem, x0_sem, q_ssem, q_rsem, qx_sem, kv_ssem, kv_rsem,
                  o_ssem, o_rsem, l_ssem, l_rsem, ob_sem, x_ssem, x_rsem):
    n_ctx, layers, rows, dim, kvh, grp, hd, pos, slots, nslot, ch = cfg
    chips = n_ctx // 2
    qw = grp * hd
    half_q = chips * qw
    half_kv = chips * hd
    xw = dim // (2 * chips)
    steps = 2 * chips + 2
    total = layers * steps
    scale = hd ** -0.5
    me = lax.axis_index('ctx')
    p = me // 2
    c = me % 2
    mate = 2 * p + (1 - c)
    far = chips // 2
    my_head = chips * c + p
    far_head = chips * c + (p + far) % chips
    near_len = 6 * pos
    my_rows = pl.ds(pl.multiple_of(c * rows, rows), rows)
    mate_rows = pl.ds(pl.multiple_of((1 - c) * rows, rows), rows)

    def issue_weights(g):
        lyr = g // steps
        j = g % steps
        slot = g % nslot

        @pl.when(g < total)
        def _():
            @pl.when(j < chips)
            def _():
                dest = (p + (j + chips // 2) % chips) % chips
                off = pl.multiple_of(c * half_q + dest * qw, 128)
                pltpu.make_async_copy(wq.at[lyr, :, pl.ds(off, qw)], wbuf.at[slot], w_sem.at[slot]).start()

            @pl.when(j == chips)
            def _():
                off = pl.multiple_of(c * half_kv, 128)
                pltpu.make_async_copy(wk.at[lyr, :, pl.ds(off, half_kv)], wbuf.at[slot], w_sem.at[slot]).start()

            @pl.when(j == chips + 1)
            def _():
                off = pl.multiple_of(c * half_kv, 128)
                pltpu.make_async_copy(wv.at[lyr, :, pl.ds(off, half_kv)], wbuf.at[slot], w_sem.at[slot]).start()

            @pl.when(j > chips + 1)
            def _():
                off = pl.multiple_of(c * (dim // 2) + (j - chips - 2) * xw, 128)
                pltpu.make_async_copy(wo.at[lyr, :, pl.ds(off, xw)], wbuf.at[slot], w_sem.at[slot]).start()

    def wait_weights(g):
        slot = g % nslot
        pltpu.make_async_copy(wq.at[0, :, pl.ds(0, qw)], wbuf.at[slot], w_sem.at[slot]).wait()
        return slot

    def raw_copies(lyr):
        return (pltpu.make_async_copy(kp.at[lyr], raw.at[0], raw_sem.at[0]),
                pltpu.make_async_copy(vp.at[lyr], raw.at[1], raw_sem.at[1]))

    def wait_kv_sent(slot):
        for t in range(2):
            full = kvsrc.at[slot, t, pl.ds(0, 6)]
            pltpu.make_async_remote_copy(full, full, kv_ssem.at[slot, t], kv_rsem.at[0, 0],
                                         device_id={'ctx': mate}, device_id_type=MESH).wait_send()

    def prep_kv(lyr, then=None):
        slot = lyr % 2
        blk = 64
        for t in range(2):
            pltpu.make_async_copy((kp, vp)[t].at[lyr], raw.at[t], raw_sem.at[t]).wait()

            def step(r, _):
                kf[...] = raw[t, pl.ds(pl.multiple_of(r * blk * kvh, 16), blk * kvh), :].astype(F32)
                for h in range(kvh):
                    kvsrc[slot, t, h, pl.ds(pl.multiple_of(r * blk, blk), blk), :] = kf[pl.ds(h, blk, stride=kvh), :].astype(BF16)
                return 0
            lax.fori_loop(0, pos // blk, step, 0)
            kvbuf[lyr, t, pl.ds(pl.multiple_of(c * pos, pos), pos), :] = kvsrc[slot, t, my_head]
            kvbuf[lyr, t, pl.ds(pl.multiple_of((6 + c) * pos, pos), pos), :] = kvsrc[slot, t, far_head]
            if then is not None:
                then(t)

        @pl.when(lyr + 1 < layers)
        def _():
            for cp in raw_copies(lyr + 1):
                cp.start()

    def send_kv(lyr, t, head, place, dev):
        slot = lyr % 2
        pltpu.make_async_remote_copy(
            kvsrc.at[slot, t, head], kvbuf.at[lyr, t, pl.ds(pl.multiple_of((place + c) * pos, pos), pos)],
            kv_ssem.at[slot, t], kv_rsem.at[lyr, t], device_id={'ctx': dev}, device_id_type=MESH).start()

    def send_kv_mate(lyr, t):
        send_kv(lyr, t, chips * (1 - c) + p, 0, mate)
        send_kv(lyr, t, chips * (1 - c) + (p + far) % chips, 6, mate)

    def send_kv_near(lyr, t, cc):
        up = (p + 1) % chips
        down = (p + chips - 1) % chips
        send_kv(lyr, t, chips * cc + up, 2, 2 * up + cc)
        send_kv(lyr, t, chips * cc + down, 4, 2 * down + cc)

    def wait_kv(lyr):
        for t in range(2):
            part = kvbuf.at[lyr, t, pl.ds(0, 6 * pos)]
            pltpu.make_async_remote_copy(part, part, kv_ssem.at[0, 0], kv_rsem.at[lyr, t],
                                         device_id={'ctx': mate}, device_id_type=MESH).wait_recv()

    def sfx_copies(lyr):
        return (pltpu.make_async_copy(ks.at[lyr], sfx.at[0], sfx_sem.at[0]),
                pltpu.make_async_copy(vs.at[lyr], sfx.at[1], sfx_sem.at[1]))

    for cp in raw_copies(0):
        cp.start()
    for g in range(nslot):
        issue_weights(jnp.int32(g))
    for cp in sfx_copies(0):
        cp.start()
    barrier = pltpu.get_barrier_semaphore()
    for j in range(1, n_ctx):
        pl.semaphore_signal(barrier, inc=1, device_id={'ctx': (me + j) % n_ctx}, device_id_type=MESH)
    xbuf[0, my_rows, :] = hid_ref[...]
    pl.semaphore_wait(barrier, n_ctx - 1)
    x0 = pltpu.make_async_remote_copy(xbuf.at[0, my_rows], xbuf.at[0, my_rows], x0_sem.at[0], x0_sem.at[1],
                                      device_id={'ctx': mate}, device_id_type=MESH)
    x0.start()

    def send_first(t):
        for cc in range(2):
            send_kv_near(jnp.int32(0), t, cc)
        send_kv_mate(jnp.int32(0), t)

    prep_kv(jnp.int32(0), send_first)
    x0.wait()

    def q_copy(kind, head):
        dest = (head + far * kind) % chips
        return pltpu.make_async_remote_copy(qkv.at[head], qall.at[kind, p], q_ssem.at[kind, head], q_rsem.at[kind, p],
                                            device_id={'ctx': 2 * dest + c}, device_id_type=MESH)

    def q_recv(kind, src):
        return pltpu.make_async_remote_copy(qkv.at[src], qall.at[kind, src], q_ssem.at[kind, src], q_rsem.at[kind, src],
                                            device_id={'ctx': mate}, device_id_type=MESH)

    def o_copy(kind, dest, cc):
        to = (my_head, far_head)[kind]
        return pltpu.make_async_remote_copy(osend.at[kind, dest, cc], orecv.at[kind, to], o_ssem.at[kind, dest, cc], o_rsem.at[kind, to],
                                            device_id={'ctx': 2 * dest + cc}, device_id_type=MESH)

    def l_copy(kind, dest, cc):
        to = (my_head, far_head)[kind]
        return pltpu.make_async_remote_copy(lsend.at[kind, dest, cc], lrecv.at[kind, to], l_ssem.at[kind, dest, cc], l_rsem.at[kind, to],
                                            device_id={'ctx': 2 * dest + cc}, device_id_type=MESH)

    def layer(lyr, _):
        cur = lyr % 2
        nxt = 1 - cur
        base = lyr * steps

        def proj(t, _):
            g = base + t
            slot = wait_weights(g)
            val = jnp.dot(xbuf[cur], wbuf[slot], preferred_element_type=F32).astype(BF16)
            dest = jnp.where(t < chips, (p + (t + chips // 2) % chips) % chips, t)
            qkv[dest] = val

            @pl.when(t < chips)
            def _():
                for kind in range(2):
                    @pl.when((dest + far * kind) % chips != p)
                    def _():
                        q_copy(kind, dest).start()

                    @pl.when((dest + far * kind) % chips == p)
                    def _():
                        qall[kind, p] = val
            issue_weights(g + nslot)
            return 0

        lax.fori_loop(0, chips + 2, proj, 0)
        qx_cp = pltpu.make_async_remote_copy(qkv.at[:, mate_rows], qx, qx_sem.at[0], qx_sem.at[1],
                                             device_id={'ctx': mate}, device_id_type=MESH)
        qx_cp.start()

        @pl.when(lyr + 1 < layers)
        def _():
            @pl.when(lyr >= 1)
            def _():
                wait_kv_sent((lyr + 1) % 2)
            prep_kv(lyr + 1)

        qx_cp.wait_recv()
        mine = c * 1
        for h in range(kvh):
            own = mine == h // chips
            hh = h % chips
            for g in range(grp):
                sel = jnp.where(own, qkv[hh, my_rows, g * hd:(g + 1) * hd].astype(F32), qx[hh, :, g * hd:(g + 1) * hd].astype(F32))
                q3[pl.ds(h * grp + g, rows, stride=kvh * grp), :] = sel
            for t in range(2):
                sel = jnp.where(own, qkv[chips + t, my_rows, hh * hd:(hh + 1) * hd].astype(F32), qx[chips + t, :, hh * hd:(hh + 1) * hd].astype(F32))
                n3[t, pl.ds(h, rows, stride=kvh), :] = sel
        kn_ref[lyr] = n3[0].astype(BF16)
        vn_ref[lyr] = n3[1].astype(BF16)
        for cp in sfx_copies(lyr):
            cp.wait()
        nh = kvh * grp
        cols = slots * kvh
        slot_id = lax.broadcasted_iota(jnp.int32, (slots, kvh, hd), 0)
        col_id = lax.broadcasted_iota(jnp.int32, (nh, cols), 1)
        row_id = lax.broadcasted_iota(jnp.int32, (nh, cols), 0)
        same = (col_id % kvh) == (row_id // grp)
        col_slot = jnp.where(same, col_id // kvh, slots + 1)
        unroll = UNROLL
        batches = rows // unroll
        early = jnp.where(lyr == 0, batches, EARLY)

        def suffix(i, _):
            bs = [i * unroll + u for u in range(unroll)]
            lns = [lens_ref[b] for b in bs]
            ats = [pl.ds(pl.multiple_of(b * nh, nh), nh) for b in bs]
            kv = []
            for b, ln in zip(bs, lns):
                hit = slot_id == ln
                for t in range(2):
                    new = n3[t, pl.ds(pl.multiple_of(b * kvh, kvh), kvh), :]
                    old = sfx[t, b].astype(F32).reshape(slots, kvh, hd)
                    kv.append(jnp.where(hit, new[None], old).reshape(cols, hd).astype(BF16))
            ss = [lax.dot_general(q3[at, :].astype(BF16), kv[2 * u], (((1,), (1,)), ((), ())), preferred_element_type=F32) * scale
                  for u, at in enumerate(ats)]
            ss = [jnp.where(col_slot <= ln, s, -jnp.inf) for s, ln in zip(ss, lns)]
            ms = [s.max(axis=-1, keepdims=True) for s in ss]
            es = [jnp.exp(s - m) for s, m in zip(ss, ms)]
            sums = [e.sum(axis=-1, keepdims=True) for e in es]
            os = [jnp.dot(e.astype(BF16), kv[2 * u + 1], preferred_element_type=F32) for u, e in enumerate(es)]
            for at, m, mass, o in zip(ats, ms, sums, os):
                o3[at, :] = o / mass
                l3[at, :] = jnp.broadcast_to(m + jnp.log(mass), (nh, hd))
            return 0

        lax.fori_loop(0, early, suffix, 0)


        def attend(kind, lo, hi, t):
            src = (p + (t + 1) % chips) % chips

            @pl.when(src != p)
            def _():
                q_recv(kind, src).wait_recv()
            qv = jnp.concatenate([qall[kind, src, cc * rows:(cc + 1) * rows, g * hd:(g + 1) * hd]
                                  for cc in range(2) for g in range(grp)], axis=0)
            n_rows = 2 * grp * rows
            mx = jnp.full((n_rows, hd), NEG, F32)
            for j in range(lo, hi, ch):
                s = lax.dot_general(qv, kvbuf[lyr, 0, j:j + ch, :], (((1,), (1,)), ((), ())), preferred_element_type=F32)
                sscr[:, j:j + ch] = s
                for b in range(ch // hd):
                    mx = jnp.maximum(mx, s[:, b * hd:(b + 1) * hd])
            m = mx.max(axis=-1, keepdims=True)
            acc = jnp.zeros((n_rows, hd), F32)
            ls = jnp.zeros((n_rows, hd), F32)
            for j in range(lo, hi, ch):
                e = jnp.exp2((sscr[:, j:j + ch] - m) * (scale * LOG2E))
                for b in range(ch // hd):
                    ls = ls + e[:, b * hd:(b + 1) * hd]
                acc = acc + jnp.dot(e.astype(BF16), kvbuf[lyr, 1, j:j + ch, :], preferred_element_type=F32)
            mass = ls.sum(axis=-1, keepdims=True)
            o = (acc / mass).astype(BF16)
            lse = jnp.broadcast_to(m * scale + jnp.log(mass), (n_rows, hd))
            per = grp * rows
            to = (my_head, far_head)[kind]
            for cc in range(2):
                dev = 2 * src + cc
                for g in range(grp):
                    osend[kind, src, cc, :, g * hd:(g + 1) * hd] = o[cc * per + g * rows: cc * per + (g + 1) * rows]
                lsend[kind, src, cc] = jnp.transpose(lse[cc * per:(cc + 1) * per])[0:8]

                @pl.when(dev != me)
                def _():
                    o_copy(kind, src, cc).start()
                    l_copy(kind, src, cc).start()

                @pl.when(dev == me)
                def _():
                    orecv[kind, to] = osend[kind, src, cc]
                    lrecv[kind, to] = lsend[kind, src, cc]

        def attend_far(t, _):
            attend(1, near_len, near_len + 2 * pos, t)
            return 0

        def attend_near(t, _):
            attend(0, 0, near_len, t)
            if PACED:
                @pl.when((lyr + 1 < layers) & (t < 4))
                def _():
                    send_kv_near(lyr + 1, t // 2, t % 2)
            return 0

        wait_kv(lyr)
        lax.fori_loop(0, chips, attend_far, 0)
        lax.fori_loop(0, chips, attend_near, 0)

        @pl.when(lyr + 1 < layers)
        def _():
            for t in range(2):
                if not PACED:
                    for cc in range(2):
                        send_kv_near(lyr + 1, t, cc)
                send_kv_mate(lyr + 1, t)

        lax.fori_loop(early, batches, suffix, 0)

        @pl.when(lyr + 1 < layers)
        def _():
            for cp in sfx_copies(lyr + 1):
                cp.start()

        for h in range(kvh):
            lps = []
            for kind in range(2):
                @pl.when((my_head, far_head)[kind] != h)
                def _():
                    pltpu.make_async_remote_copy(osend.at[0, 0, 0], orecv.at[kind, h], o_ssem.at[0, 0, 0], o_rsem.at[kind, h],
                                                 device_id={'ctx': mate}, device_id_type=MESH).wait_recv()
                    pltpu.make_async_remote_copy(lsend.at[0, 0, 0], lrecv.at[kind, h], l_ssem.at[0, 0, 0], l_rsem.at[kind, h],
                                                 device_id={'ctx': mate}, device_id_type=MESH).wait_recv()
                lps.append(jnp.transpose(jnp.concatenate([lrecv[kind, h]] * (hd // 8), axis=0)))
            for g in range(grp):
                hx = h * grp + g
                la, lb = [lp[g * rows:(g + 1) * rows] for lp in lps]
                ls = l3[pl.ds(hx, rows, stride=kvh * grp), :]
                os = o3[pl.ds(hx, rows, stride=kvh * grp), :]
                top = jnp.maximum(jnp.maximum(la, lb), ls)
                wa = jnp.exp(la - top)
                wb = jnp.exp(lb - top)
                ws = jnp.exp(ls - top)
                mix = (wa * orecv[0, h, :, g * hd:(g + 1) * hd].astype(F32) + wb * orecv[1, h, :, g * hd:(g + 1) * hd].astype(F32)
                       + ws * os) / (wa + wb + ws)
                obuf[my_rows, hx * hd:(hx + 1) * hd] = mix.astype(BF16)
        ob = pltpu.make_async_remote_copy(obuf.at[my_rows], obuf.at[my_rows], ob_sem.at[0], ob_sem.at[1],
                                          device_id={'ctx': mate}, device_id_type=MESH)
        ob.start()
        ob.wait_recv()

        def x_copy(n):
            col = pl.ds(pl.multiple_of(c * (dim // 2) + n * xw, 128), xw)
            return pltpu.make_async_remote_copy(xbuf.at[nxt, :, col], xbuf.at[nxt, :, col], x_ssem.at[n], x_rsem.at[n],
                                                device_id={'ctx': mate}, device_id_type=MESH)

        def outp(n, _):
            g = base + chips + 2 + n
            slot = wait_weights(g)
            upd = jnp.dot(obuf[...], wbuf[slot], preferred_element_type=F32).astype(BF16)
            col = pl.ds(pl.multiple_of(c * (dim // 2) + n * xw, 128), xw)
            xbuf[nxt, :, col] = (xbuf[cur, :, col].astype(F32) + upd.astype(F32)).astype(BF16)
            x_copy(n).start()
            issue_weights(g + nslot)
            return 0

        lax.fori_loop(0, chips, outp, 0)

        qx_cp.wait_send()
        ob.wait_send()
        for kind in range(2):
            for t in range(chips):
                @pl.when(p != (t + far * kind) % chips)
                def _():
                    q_copy(kind, t).wait_send()
                for cc in range(2):
                    @pl.when(me != 2 * t + cc)
                    def _():
                        o_copy(kind, t, cc).wait_send()
                        l_copy(kind, t, cc).wait_send()
        for n in range(chips):
            x_copy(n).wait()
        return 0

    lax.fori_loop(0, layers, layer, 0)
    for back in range(min(2, layers)):
        wait_kv_sent((layers - 1 - back) % 2)
    out_ref[...] = xbuf[layers % 2, my_rows, :]


def insert_kernel(lens_ref, hid_ref, kn_ref, vn_ref, ks_ref, vs_ref, ho_ref, ko_ref, vo_ref,
                  hid, new, buf, h_sem, n_sem, in_sem, out_sem):
    layers, rows = ks_ref.shape[:2]
    sides = ((kn_ref, ks_ref, ko_ref), (vn_ref, vs_ref, vo_ref))
    news = [pltpu.make_async_copy(sides[t][0], new.at[t], n_sem.at[t]) for t in range(2)]
    loads = [(lyr, t, pltpu.make_async_copy(sides[t][1].at[lyr], buf.at[lyr, t], in_sem.at[lyr, t]))
             for lyr in range(layers) for t in range(2)]
    h_in = pltpu.make_async_copy(hid_ref, hid, h_sem.at[0])
    h_out = pltpu.make_async_copy(hid, ho_ref, h_sem.at[1])
    for cp in news:
        cp.start()
    for _, _, cp in loads:
        cp.start()
    h_in.start()
    for cp in news:
        cp.wait()
    stores = []
    for lyr, t, cp in loads:
        cp.wait()
        for b in range(rows):
            buf[lyr, t, b, lens_ref[b]] = new[t, lyr, b]
        out = pltpu.make_async_copy(buf.at[lyr, t], sides[t][2].at[lyr], out_sem.at[lyr, t])
        out.start()
        stores.append(out)
    h_in.wait()
    h_out.start()
    for out in stores:
        out.wait()
    h_out.wait()


def solution(mesh):
    n_ctx = mesh.shape['ctx']
    home_axes = ('data', 'ctx')
    row_spec = P(home_axes, None)
    lens_spec = P(home_axes)
    whole_spec = P()
    prefix_spec = P(None, home_axes, None, None)
    cache_spec = P(None, home_axes, None, None, None)

    def local_step(hidden, seq_lens, w_query, w_key, w_value, w_out, k_prefix, v_prefix, k_suffix, v_suffix):
        layers, pos, kvh, hd = k_prefix.shape
        rows, dim = hidden.shape
        slots = k_suffix.shape[2]
        grp = w_query.shape[2] // (kvh * hd)
        chips = n_ctx // 2
        qw = grp * hd
        nslot = 7
        ch = min(1024, 2 * pos)
        cfg = (n_ctx, layers, rows, dim, kvh, grp, hd, pos, slots, nslot, ch)
        assert chips == 4 and kvh == n_ctx and chips * hd == qw and dim // n_ctx == qw and grp * rows == hd
        nh = kvh * grp
        vmem, anys, smem = pltpu.VMEM, pl.ANY, pltpu.SMEM
        hidden_out, k_new, v_new = pl.pallas_call(
            functools.partial(decode_kernel, cfg),
            out_shape=(jax.ShapeDtypeStruct((rows, dim), BF16),
                       jax.ShapeDtypeStruct((layers, rows * kvh, hd), BF16),
                       jax.ShapeDtypeStruct((layers, rows * kvh, hd), BF16)),
            in_specs=[pl.BlockSpec(memory_space=smem), pl.BlockSpec(memory_space=vmem)] + [pl.BlockSpec(memory_space=anys)] * 8,
            out_specs=[pl.BlockSpec(memory_space=vmem)] * 3,
            scratch_shapes=[
                vmem((nslot, dim, qw), BF16),
                vmem((2, 2 * rows, dim), BF16),
                vmem((chips + 2, 2 * rows, qw), BF16),
                vmem((chips + 2, rows, qw), BF16),
                vmem((2, chips, 2 * rows, qw), BF16),
                vmem((2, pos * kvh, hd), BF16),
                vmem((64 * kvh, hd), F32),
                vmem((2, 2, kvh, pos, hd), BF16),
                vmem((layers, 2, n_ctx * pos, hd), BF16),
                vmem((2, rows, slots * kvh, hd), BF16),
                vmem((2 * grp * rows, n_ctx * pos), F32),
                vmem((2, chips, 2, rows, qw), BF16),
                vmem((2, chips, 2, 8, hd), F32),
                vmem((2, kvh, rows, qw), BF16),
                vmem((2, kvh, 8, hd), F32),
                vmem((rows * nh, hd), F32),
                vmem((2, rows * kvh, hd), F32),
                vmem((rows * nh, hd), F32),
                vmem((rows * nh, hd), F32),
                vmem((2 * rows, nh * hd), BF16),
                pltpu.SemaphoreType.DMA((nslot,)),
                pltpu.SemaphoreType.DMA((2,)),
                pltpu.SemaphoreType.DMA((2,)),
                pltpu.SemaphoreType.DMA((2,)),
                pltpu.SemaphoreType.DMA((2, chips)),
                pltpu.SemaphoreType.DMA((2, chips)),
                pltpu.SemaphoreType.DMA((2,)),
                pltpu.SemaphoreType.DMA((2, 2)),
                pltpu.SemaphoreType.DMA((layers, 2)),
                pltpu.SemaphoreType.DMA((2, chips, 2)),
                pltpu.SemaphoreType.DMA((2, kvh)),
                pltpu.SemaphoreType.DMA((2, chips, 2)),
                pltpu.SemaphoreType.DMA((2, kvh)),
                pltpu.SemaphoreType.DMA((2,)),
                pltpu.SemaphoreType.DMA((chips,)),
                pltpu.SemaphoreType.DMA((chips,)),
            ],
            compiler_params=pltpu.CompilerParams(collective_id=0, has_side_effects=True, vmem_limit_bytes=67043328),
            name='decode_layers',
        )(seq_lens, hidden, w_query, w_key, w_value, w_out,
          k_prefix.reshape(layers, pos * kvh, hd), v_prefix.reshape(layers, pos * kvh, hd),
          k_suffix.reshape(layers, rows, slots * kvh, hd), v_suffix.reshape(layers, rows, slots * kvh, hd))
        hidden_out, k_out, v_out = pl.pallas_call(
            insert_kernel,
            out_shape=(jax.ShapeDtypeStruct((rows, dim), BF16), jax.ShapeDtypeStruct(k_suffix.shape, BF16),
                       jax.ShapeDtypeStruct(v_suffix.shape, BF16)),
            in_specs=[pl.BlockSpec(memory_space=smem)] + [pl.BlockSpec(memory_space=anys)] * 5,
            out_specs=[pl.BlockSpec(memory_space=anys)] * 3,
            scratch_shapes=[
                vmem((rows, dim), BF16),
                vmem((2, layers, rows, kvh, hd), BF16),
                vmem((layers, 2, rows, slots, kvh, hd), BF16),
                pltpu.SemaphoreType.DMA((2,)),
                pltpu.SemaphoreType.DMA((2,)),
                pltpu.SemaphoreType.DMA((layers, 2)),
                pltpu.SemaphoreType.DMA((layers, 2)),
            ],
            compiler_params=pltpu.CompilerParams(vmem_limit_bytes=67043328),
            name='insert_rows',
        )(seq_lens, hidden_out, k_new.reshape(layers, rows, kvh, hd), v_new.reshape(layers, rows, kvh, hd), k_suffix, v_suffix)
        return hidden_out, k_out, v_out

    return jax.shard_map(local_step, mesh=mesh, in_specs=(row_spec, lens_spec, whole_spec, whole_spec, whole_spec, whole_spec, prefix_spec, prefix_spec, cache_spec, cache_spec), out_specs=(row_spec, cache_spec, cache_spec), check_vma=False)
```

```python
import functools
import math

import jax
import jax.numpy as jnp
from jax import lax
from jax.experimental import pallas as pl
from jax.experimental.pallas import tpu as pltpu
from jax.sharding import PartitionSpec as P

MESH = pl.DeviceIdType.MESH
F32 = jnp.float32
BF16 = jnp.bfloat16
NEG = -1e30
UNROLL = 8
EARLY = 2
CHUNK = 1024
LOG2E = 1.4426950408889634


def decode_kernel(cfg, lens_ref, hid_ref, wq, wk, wv, wo, kp, vp, ks, vs,
                  out_ref, kn_ref, vn_ref,
                  wbuf, xbuf, qkv, qx, qall, raw, kf, kvsrc, kvbuf, sfx, sscr, mscr, osend, lsend, orecv, lrecv,
                  q3, n3, o3, l3, obuf,
                  w_sem, raw_sem, sfx_sem, x0_sem, q_ssem, q_rsem, qx_sem, kv_ssem, kv_rsem, kvm_rsem,
                  o_ssem, o_rsem, l_ssem, l_rsem, ob_sem, x_ssem, x_rsem):
    n_ctx, layers, rows, dim, kvh, grp, hd, pos, slots, nslot, ch = cfg
    chips = n_ctx // 2
    qw = grp * hd
    half_q = chips * qw
    half_kv = chips * hd
    xw = dim // (2 * chips)
    steps = 2 * chips + 2
    total = layers * steps
    scale = hd ** -0.5
    me = lax.axis_index('ctx')
    p = me // 2
    c = me % 2
    mate = 2 * p + (1 - c)
    far = chips // 2
    my_head = chips * c + p
    far_head = chips * c + (p + far) % chips
    near_len = 6 * pos
    my_rows = pl.ds(pl.multiple_of(c * rows, rows), rows)
    mate_rows = pl.ds(pl.multiple_of((1 - c) * rows, rows), rows)

    def issue_weights(g):
        lyr = g // steps
        j = g % steps
        slot = g % nslot

        @pl.when(g < total)
        def _():
            @pl.when(j < chips)
            def _():
                dest = (p + (j + chips // 2) % chips) % chips
                off = pl.multiple_of(c * half_q + dest * qw, 128)
                pltpu.make_async_copy(wq.at[lyr, :, pl.ds(off, qw)], wbuf.at[slot], w_sem.at[slot]).start()

            @pl.when(j == chips)
            def _():
                off = pl.multiple_of(c * half_kv, 128)
                pltpu.make_async_copy(wk.at[lyr, :, pl.ds(off, half_kv)], wbuf.at[slot], w_sem.at[slot]).start()

            @pl.when(j == chips + 1)
            def _():
                off = pl.multiple_of(c * half_kv, 128)
                pltpu.make_async_copy(wv.at[lyr, :, pl.ds(off, half_kv)], wbuf.at[slot], w_sem.at[slot]).start()

            @pl.when(j > chips + 1)
            def _():
                off = pl.multiple_of(c * (dim // 2) + (j - chips - 2) * xw, 128)
                pltpu.make_async_copy(wo.at[lyr, :, pl.ds(off, xw)], wbuf.at[slot], w_sem.at[slot]).start()

    def wait_weights(g):
        slot = g % nslot
        pltpu.make_async_copy(wq.at[0, :, pl.ds(0, qw)], wbuf.at[slot], w_sem.at[slot]).wait()
        return slot

    def raw_copies(lyr):
        return (pltpu.make_async_copy(kp.at[lyr], raw.at[0], raw_sem.at[0]),
                pltpu.make_async_copy(vp.at[lyr], raw.at[1], raw_sem.at[1]))

    def wait_kv_sent(slot, t):
        full = kvsrc.at[slot, t, pl.ds(0, 6)]
        pltpu.make_async_remote_copy(full, full, kv_ssem.at[slot, t], kv_rsem.at[0, 0],
                                     device_id={'ctx': mate}, device_id_type=MESH).wait_send()

    def prep_kv(lyr, t):
        slot = lyr % 2
        blk = 64
        pltpu.make_async_copy((kp, vp)[t].at[lyr], raw.at[t], raw_sem.at[t]).wait()

        def step(r, _):
            kf[...] = raw[t, pl.ds(pl.multiple_of(r * blk * kvh, 16), blk * kvh), :].astype(F32)
            for h in range(kvh):
                kvsrc[slot, t, h, pl.ds(pl.multiple_of(r * blk, blk), blk), :] = kf[pl.ds(h, blk, stride=kvh), :].astype(BF16)
            return 0
        lax.fori_loop(0, pos // blk, step, 0)
        kvbuf[lyr, t, pl.ds(pl.multiple_of(c * pos, pos), pos), :] = kvsrc[slot, t, my_head]
        kvbuf[lyr, t, pl.ds(pl.multiple_of((6 + c) * pos, pos), pos), :] = kvsrc[slot, t, far_head]

        @pl.when(lyr + 1 < layers)
        def _():
            pltpu.make_async_copy((kp, vp)[t].at[lyr + 1], raw.at[t], raw_sem.at[t]).start()

    def send_kv(lyr, t, head, place, dev, sem):
        slot = lyr % 2
        pltpu.make_async_remote_copy(
            kvsrc.at[slot, t, head], kvbuf.at[lyr, t, pl.ds(pl.multiple_of((place + c) * pos, pos), pos)],
            kv_ssem.at[slot, t], sem.at[lyr, t], device_id={'ctx': dev}, device_id_type=MESH).start()

    def send_kv_mate(lyr, t):
        send_kv(lyr, t, chips * (1 - c) + p, 0, mate, kvm_rsem)
        send_kv(lyr, t, chips * (1 - c) + (p + far) % chips, 6, mate, kvm_rsem)

    def send_kv_near(lyr, t, cc):
        up = (p + 1) % chips
        down = (p + chips - 1) % chips
        send_kv(lyr, t, chips * cc + up, 2, 2 * up + cc, kv_rsem)
        send_kv(lyr, t, chips * cc + down, 4, 2 * down + cc, kv_rsem)

    def wait_kv(lyr, t, sem, count):
        part = kvbuf.at[lyr, t, pl.ds(0, count * pos)]
        pltpu.make_async_remote_copy(part, part, kv_ssem.at[0, 0], sem.at[lyr, t],
                                     device_id={'ctx': mate}, device_id_type=MESH).wait_recv()

    def sfx_copies(lyr):
        return (pltpu.make_async_copy(ks.at[lyr], sfx.at[0], sfx_sem.at[0]),
                pltpu.make_async_copy(vs.at[lyr], sfx.at[1], sfx_sem.at[1]))

    for cp in raw_copies(0):
        cp.start()
    issue_weights(jnp.int32(0))
    barrier = pltpu.get_barrier_semaphore()
    for j in range(1, n_ctx):
        pl.semaphore_signal(barrier, inc=1, device_id={'ctx': (me + j) % n_ctx}, device_id_type=MESH)
    xbuf[0, my_rows, :] = hid_ref[...]
    pl.semaphore_wait(barrier, n_ctx - 1)
    x0 = pltpu.make_async_remote_copy(xbuf.at[0, my_rows], xbuf.at[0, my_rows], x0_sem.at[0], x0_sem.at[1],
                                      device_id={'ctx': mate}, device_id_type=MESH)
    x0.start()
    for t in range(2):
        prep_kv(jnp.int32(0), t)
        if t == 0:
            for g in range(1, nslot):
                issue_weights(jnp.int32(g))
            for cc in range(2):
                send_kv_near(jnp.int32(0), t, cc)
        send_kv_mate(jnp.int32(0), t)
    for cp in sfx_copies(0):
        cp.start()
    x0.wait()

    def q_copy(kind, head):
        dest = (head + far * kind) % chips
        return pltpu.make_async_remote_copy(qkv.at[head], qall.at[kind, p], q_ssem.at[kind, head], q_rsem.at[kind, p],
                                            device_id={'ctx': 2 * dest + c}, device_id_type=MESH)

    def q_recv(kind, src):
        return pltpu.make_async_remote_copy(qkv.at[src], qall.at[kind, src], q_ssem.at[kind, src], q_rsem.at[kind, src],
                                            device_id={'ctx': mate}, device_id_type=MESH)

    def o_copy(kind, dest, cc):
        to = (my_head, far_head)[kind]
        return pltpu.make_async_remote_copy(osend.at[kind, dest, cc], orecv.at[kind, to], o_ssem.at[kind, dest, cc], o_rsem.at[kind, to],
                                            device_id={'ctx': 2 * dest + cc}, device_id_type=MESH)

    def l_copy(kind, dest, cc):
        to = (my_head, far_head)[kind]
        return pltpu.make_async_remote_copy(lsend.at[kind, dest, cc], lrecv.at[kind, to], l_ssem.at[kind, dest, cc], l_rsem.at[kind, to],
                                            device_id={'ctx': 2 * dest + cc}, device_id_type=MESH)

    def layer(lyr, _):
        cur = lyr % 2
        nxt = 1 - cur
        base = lyr * steps

        def proj(t, _):
            g = base + t
            slot = wait_weights(g)
            val = jnp.dot(xbuf[cur], wbuf[slot], preferred_element_type=F32).astype(BF16)
            dest = jnp.where(t < chips, (p + (t + chips // 2) % chips) % chips, t)
            qkv[dest] = val

            @pl.when(t < chips)
            def _():
                for kind in range(2):
                    @pl.when((dest + far * kind) % chips != p)
                    def _():
                        q_copy(kind, dest).start()

                    @pl.when((dest + far * kind) % chips == p)
                    def _():
                        qall[kind, p] = val
            issue_weights(g + nslot)
            return 0

        lax.fori_loop(0, chips + 2, proj, 0)
        qx_cp = pltpu.make_async_remote_copy(qkv.at[:, mate_rows], qx, qx_sem.at[0], qx_sem.at[1],
                                             device_id={'ctx': mate}, device_id_type=MESH)
        qx_cp.start()

        @pl.when(lyr == 0)
        def _():
            for cc in range(2):
                send_kv_near(lyr, 1, cc)

        @pl.when((lyr == 0) & (layers > 1))
        def _():
            prep_kv(lyr + 1, 0)
            prep_kv(lyr + 1, 1)

        n_rows = 2 * grp * rows
        per = grp * rows
        rate = scale * LOG2E

        def src_at(kind, t):
            return (p + chips - t) % chips if kind else (p + t + 1) % chips

        def take_q(kind, t):
            src = src_at(kind, t)

            @pl.when(src != p)
            def _():
                q_recv(kind, src).wait_recv()
            return jnp.concatenate([qall[kind, src, cc * rows:(cc + 1) * rows, g * hd:(g + 1) * hd]
                                    for cc in range(2) for g in range(grp)], axis=0)

        def block(kind, lo, hi, t, score, value):
            old = mscr[...] if value else None
            qv = take_q(kind, t) if score else None
            if score:
                mx = jnp.full((n_rows, hd), NEG, F32)
            if value:
                acc = jnp.zeros((n_rows, hd), F32)
                ls = jnp.zeros((n_rows, hd), F32)
            for j in range(lo, hi, ch):
                if value:
                    e = jnp.exp2((sscr[:, j:j + ch] - old[:, 0:1]) * rate)
                if score:
                    s = lax.dot_general(qv, kvbuf[lyr, 0, j:j + ch, :], (((1,), (1,)), ((), ())), preferred_element_type=F32)
                    sscr[:, j:j + ch] = s
                if value:
                    for b in range(ch // hd):
                        ls = ls + e[:, b * hd:(b + 1) * hd]
                    acc = acc + jnp.dot(e.astype(BF16), kvbuf[lyr, 1, j:j + ch, :], preferred_element_type=F32)
                if score:
                    for b in range(ch // hd):
                        mx = jnp.maximum(mx, s[:, b * hd:(b + 1) * hd])
            if score:
                mscr[...] = jnp.broadcast_to(mx.max(axis=-1, keepdims=True), (n_rows, hd))
            if value:
                src = src_at(kind, t - 1)
                to = (my_head, far_head)[kind]
                mass = ls.sum(axis=-1, keepdims=True)
                o = (acc / mass).astype(BF16)
                lse = old * scale + jnp.log(mass)
                for cc in range(2):
                    dev = 2 * src + cc
                    for g in range(grp):
                        osend[kind, src, cc, :, g * hd:(g + 1) * hd] = o[cc * per + g * rows: cc * per + (g + 1) * rows]
                    lsend[kind, src, cc] = jnp.transpose(lse[cc * per:(cc + 1) * per])[0:8]

                    @pl.when(dev != me)
                    def _():
                        o_copy(kind, src, cc).start()
                        l_copy(kind, src, cc).start()

                    @pl.when(dev == me)
                    def _():
                        orecv[kind, to] = osend[kind, src, cc]
                        lrecv[kind, to] = lsend[kind, src, cc]

        def attention(kind, first, lo, hi):
            block(kind, lo, hi, first, True, False)

            def both(t, _):
                block(kind, lo, hi, t, True, True)
                return 0
            lax.fori_loop(first + 1, chips, both, 0)
            block(kind, lo, hi, chips, False, True)

        far_part = (near_len, near_len + 2 * pos)
        near_part = (0, near_len)
        wait_kv(lyr, 0, kvm_rsem, 2)
        wait_kv(lyr, 1, kvm_rsem, 2)
        block(1, *far_part, 0, True, False)
        block(1, *far_part, 1, False, True)

        qx_cp.wait_recv()
        mine = c * 1
        for h in range(kvh):
            own = mine == h // chips
            hh = h % chips
            for g in range(grp):
                sel = jnp.where(own, qkv[hh, my_rows, g * hd:(g + 1) * hd].astype(F32), qx[hh, :, g * hd:(g + 1) * hd].astype(F32))
                q3[pl.ds(h * grp + g, rows, stride=kvh * grp), :] = sel
            for t in range(2):
                sel = jnp.where(own, qkv[chips + t, my_rows, hh * hd:(hh + 1) * hd].astype(F32), qx[chips + t, :, hh * hd:(hh + 1) * hd].astype(F32))
                n3[t, pl.ds(h, rows, stride=kvh), :] = sel
        kn_ref[lyr] = n3[0].astype(BF16)
        vn_ref[lyr] = n3[1].astype(BF16)
        for cp in sfx_copies(lyr):
            cp.wait()
        nh = kvh * grp
        cols = slots * kvh
        slot_id = lax.broadcasted_iota(jnp.int32, (slots, kvh, hd), 0)
        col_id = lax.broadcasted_iota(jnp.int32, (nh, cols), 1)
        row_id = lax.broadcasted_iota(jnp.int32, (nh, cols), 0)
        same = (col_id % kvh) == (row_id // grp)
        col_slot = jnp.where(same, col_id // kvh, slots + 1)
        unroll = UNROLL
        batches = rows // unroll
        early = jnp.where(lyr == 0, batches, EARLY)

        def suffix(i, _):
            bs = [i * unroll + u for u in range(unroll)]
            lns = [lens_ref[b] for b in bs]
            ats = [pl.ds(pl.multiple_of(b * nh, nh), nh) for b in bs]
            kv = []
            for b, ln in zip(bs, lns):
                hit = slot_id == ln
                for t in range(2):
                    new = n3[t, pl.ds(pl.multiple_of(b * kvh, kvh), kvh), :]
                    old = sfx[t, b].astype(F32).reshape(slots, kvh, hd)
                    kv.append(jnp.where(hit, new[None], old).reshape(cols, hd).astype(BF16))
            ss = [lax.dot_general(q3[at, :].astype(BF16), kv[2 * u], (((1,), (1,)), ((), ())), preferred_element_type=F32) * scale
                  for u, at in enumerate(ats)]
            ss = [jnp.where(col_slot <= ln, s, -jnp.inf) for s, ln in zip(ss, lns)]
            ms = [s.max(axis=-1, keepdims=True) for s in ss]
            es = [jnp.exp(s - m) for s, m in zip(ss, ms)]
            sums = [e.sum(axis=-1, keepdims=True) for e in es]
            os = [jnp.dot(e.astype(BF16), kv[2 * u + 1], preferred_element_type=F32) for u, e in enumerate(es)]
            for at, m, mass, o in zip(ats, ms, sums, os):
                o3[at, :] = o / mass
                l3[at, :] = jnp.broadcast_to(m + jnp.log(mass), (nh, hd))
            return 0

        lax.fori_loop(0, early, suffix, 0)


        attention(1, 1, *far_part)
        wait_kv(lyr, 0, kv_rsem, 4)
        wait_kv(lyr, 1, kv_rsem, 4)
        attention(0, 0, *near_part)

        @pl.when(lyr + 1 < layers)
        def _():
            for t in range(2):
                for cc in range(2):
                    send_kv_near(lyr + 1, t, cc)
                send_kv_mate(lyr + 1, t)

        lax.fori_loop(early, batches, suffix, 0)

        @pl.when(lyr + 1 < layers)
        def _():
            for cp in sfx_copies(lyr + 1):
                cp.start()

        def arrived(kind, h):
            @pl.when((my_head, far_head)[kind] != h)
            def _():
                pltpu.make_async_remote_copy(osend.at[0, 0, 0], orecv.at[kind, h], o_ssem.at[0, 0, 0], o_rsem.at[kind, h],
                                             device_id={'ctx': mate}, device_id_type=MESH).wait_recv()
                pltpu.make_async_remote_copy(lsend.at[0, 0, 0], lrecv.at[kind, h], l_ssem.at[0, 0, 0], l_rsem.at[kind, h],
                                             device_id={'ctx': mate}, device_id_type=MESH).wait_recv()
            return jnp.transpose(jnp.concatenate([lrecv[kind, h]] * (hd // 8), axis=0))

        for kind in (1, 0):
            for h in range(kvh):
                lp = arrived(kind, h)
                for g in range(grp):
                    hx = h * grp + g
                    at = pl.ds(hx, rows, stride=kvh * grp)
                    la = lp[g * rows:(g + 1) * rows]
                    ls = l3[at, :]
                    top = jnp.maximum(la, ls)
                    wa = jnp.exp(la - top)
                    ws = jnp.exp(ls - top)
                    both_mass = wa + ws
                    mix = (wa * orecv[kind, h, :, g * hd:(g + 1) * hd].astype(F32) + ws * o3[at, :]) / both_mass
                    if kind:
                        o3[at, :] = mix
                        l3[at, :] = top + jnp.log(both_mass)
                    else:
                        obuf[my_rows, hx * hd:(hx + 1) * hd] = mix.astype(BF16)
        ob = pltpu.make_async_remote_copy(obuf.at[my_rows], obuf.at[my_rows], ob_sem.at[0], ob_sem.at[1],
                                          device_id={'ctx': mate}, device_id_type=MESH)
        ob.start()

        def prep_ahead(t):
            @pl.when(lyr + 2 < layers)
            def _():
                wait_kv_sent(lyr % 2, t)
                prep_kv(lyr + 2, t)

        prep_ahead(0)
        ob.wait_recv()

        def x_copy(n):
            col = pl.ds(pl.multiple_of(c * (dim // 2) + n * xw, 128), xw)
            return pltpu.make_async_remote_copy(xbuf.at[nxt, :, col], xbuf.at[nxt, :, col], x_ssem.at[n], x_rsem.at[n],
                                                device_id={'ctx': mate}, device_id_type=MESH)

        def outp(n, _):
            g = base + chips + 2 + n
            slot = wait_weights(g)
            upd = jnp.dot(obuf[...], wbuf[slot], preferred_element_type=F32).astype(BF16)
            col = pl.ds(pl.multiple_of(c * (dim // 2) + n * xw, 128), xw)
            xbuf[nxt, :, col] = (xbuf[cur, :, col].astype(F32) + upd.astype(F32)).astype(BF16)
            x_copy(n).start()
            issue_weights(g + nslot)
            return 0

        lax.fori_loop(0, chips, outp, 0)
        prep_ahead(1)

        qx_cp.wait_send()
        ob.wait_send()
        for kind in range(2):
            for t in range(chips):
                @pl.when(p != (t + far * kind) % chips)
                def _():
                    q_copy(kind, t).wait_send()
                for cc in range(2):
                    @pl.when(me != 2 * t + cc)
                    def _():
                        o_copy(kind, t, cc).wait_send()
                        l_copy(kind, t, cc).wait_send()
        for n in range(chips):
            x_copy(n).wait()
        return 0

    lax.fori_loop(0, layers, layer, 0)
    for back in range(min(2, layers)):
        for t in range(2):
            wait_kv_sent((layers - 1 - back) % 2, t)
    out_ref[...] = xbuf[layers % 2, my_rows, :]


def insert_kernel(lens_ref, hid_ref, kn_ref, vn_ref, ks_ref, vs_ref, ho_ref, ko_ref, vo_ref,
                  hid, new, buf, h_sem, n_sem, in_sem, out_sem):
    layers, rows = ks_ref.shape[:2]
    sides = ((kn_ref, ks_ref, ko_ref), (vn_ref, vs_ref, vo_ref))
    news = [pltpu.make_async_copy(sides[t][0], new.at[t], n_sem.at[t]) for t in range(2)]
    loads = [(lyr, t, pltpu.make_async_copy(sides[t][1].at[lyr], buf.at[lyr, t], in_sem.at[lyr, t]))
             for lyr in range(layers) for t in range(2)]
    h_in = pltpu.make_async_copy(hid_ref, hid, h_sem.at[0])
    h_out = pltpu.make_async_copy(hid, ho_ref, h_sem.at[1])
    for cp in news:
        cp.start()
    for _, _, cp in loads:
        cp.start()
    h_in.start()
    for cp in news:
        cp.wait()
    stores = []
    for lyr, t, cp in loads:
        cp.wait()
        for b in range(rows):
            buf[lyr, t, b, lens_ref[b]] = new[t, lyr, b]
        out = pltpu.make_async_copy(buf.at[lyr, t], sides[t][2].at[lyr], out_sem.at[lyr, t])
        out.start()
        stores.append(out)
    h_in.wait()
    h_out.start()
    for out in stores:
        out.wait()
    h_out.wait()


def solution(mesh):
    n_ctx = mesh.shape['ctx']
    home_axes = ('data', 'ctx')
    row_spec = P(home_axes, None)
    lens_spec = P(home_axes)
    whole_spec = P()
    prefix_spec = P(None, home_axes, None, None)
    cache_spec = P(None, home_axes, None, None, None)

    def local_step(hidden, seq_lens, w_query, w_key, w_value, w_out, k_prefix, v_prefix, k_suffix, v_suffix):
        layers, pos, kvh, hd = k_prefix.shape
        rows, dim = hidden.shape
        slots = k_suffix.shape[2]
        grp = w_query.shape[2] // (kvh * hd)
        chips = n_ctx // 2
        qw = grp * hd
        nslot = 7
        ch = min(CHUNK, 2 * pos)
        cfg = (n_ctx, layers, rows, dim, kvh, grp, hd, pos, slots, nslot, ch)
        assert chips == 4 and kvh == n_ctx and chips * hd == qw and dim // n_ctx == qw and grp * rows == hd
        nh = kvh * grp
        vmem, anys, smem = pltpu.VMEM, pl.ANY, pltpu.SMEM
        hidden_out, k_new, v_new = pl.pallas_call(
            functools.partial(decode_kernel, cfg),
            out_shape=(jax.ShapeDtypeStruct((rows, dim), BF16),
                       jax.ShapeDtypeStruct((layers, rows * kvh, hd), BF16),
                       jax.ShapeDtypeStruct((layers, rows * kvh, hd), BF16)),
            in_specs=[pl.BlockSpec(memory_space=smem), pl.BlockSpec(memory_space=vmem)] + [pl.BlockSpec(memory_space=anys)] * 8,
            out_specs=[pl.BlockSpec(memory_space=vmem)] * 3,
            scratch_shapes=[
                vmem((nslot, dim, qw), BF16),
                vmem((2, 2 * rows, dim), BF16),
                vmem((chips + 2, 2 * rows, qw), BF16),
                vmem((chips + 2, rows, qw), BF16),
                vmem((2, chips, 2 * rows, qw), BF16),
                vmem((2, pos * kvh, hd), BF16),
                vmem((64 * kvh, hd), F32),
                vmem((2, 2, kvh, pos, hd), BF16),
                vmem((layers, 2, n_ctx * pos, hd), BF16),
                vmem((2, rows, slots * kvh, hd), BF16),
                vmem((2 * grp * rows, n_ctx * pos), F32),
                vmem((2 * grp * rows, hd), F32),
                vmem((2, chips, 2, rows, qw), BF16),
                vmem((2, chips, 2, 8, hd), F32),
                vmem((2, kvh, rows, qw), BF16),
                vmem((2, kvh, 8, hd), F32),
                vmem((rows * nh, hd), F32),
                vmem((2, rows * kvh, hd), F32),
                vmem((rows * nh, hd), F32),
                vmem((rows * nh, hd), F32),
                vmem((2 * rows, nh * hd), BF16),
                pltpu.SemaphoreType.DMA((nslot,)),
                pltpu.SemaphoreType.DMA((2,)),
                pltpu.SemaphoreType.DMA((2,)),
                pltpu.SemaphoreType.DMA((2,)),
                pltpu.SemaphoreType.DMA((2, chips)),
                pltpu.SemaphoreType.DMA((2, chips)),
                pltpu.SemaphoreType.DMA((2,)),
                pltpu.SemaphoreType.DMA((2, 2)),
                pltpu.SemaphoreType.DMA((layers, 2)),
                pltpu.SemaphoreType.DMA((layers, 2)),
                pltpu.SemaphoreType.DMA((2, chips, 2)),
                pltpu.SemaphoreType.DMA((2, kvh)),
                pltpu.SemaphoreType.DMA((2, chips, 2)),
                pltpu.SemaphoreType.DMA((2, kvh)),
                pltpu.SemaphoreType.DMA((2,)),
                pltpu.SemaphoreType.DMA((chips,)),
                pltpu.SemaphoreType.DMA((chips,)),
            ],
            compiler_params=pltpu.CompilerParams(collective_id=0, has_side_effects=True, vmem_limit_bytes=67043328),
            name='decode_layers',
        )(seq_lens, hidden, w_query, w_key, w_value, w_out,
          k_prefix.reshape(layers, pos * kvh, hd), v_prefix.reshape(layers, pos * kvh, hd),
          k_suffix.reshape(layers, rows, slots * kvh, hd), v_suffix.reshape(layers, rows, slots * kvh, hd))
        hidden_out, k_out, v_out = pl.pallas_call(
            insert_kernel,
            out_shape=(jax.ShapeDtypeStruct((rows, dim), BF16), jax.ShapeDtypeStruct(k_suffix.shape, BF16),
                       jax.ShapeDtypeStruct(v_suffix.shape, BF16)),
            in_specs=[pl.BlockSpec(memory_space=smem)] + [pl.BlockSpec(memory_space=anys)] * 5,
            out_specs=[pl.BlockSpec(memory_space=anys)] * 3,
            scratch_shapes=[
                vmem((rows, dim), BF16),
                vmem((2, layers, rows, kvh, hd), BF16),
                vmem((layers, 2, rows, slots, kvh, hd), BF16),
                pltpu.SemaphoreType.DMA((2,)),
                pltpu.SemaphoreType.DMA((2,)),
                pltpu.SemaphoreType.DMA((layers, 2)),
                pltpu.SemaphoreType.DMA((layers, 2)),
            ],
            compiler_params=pltpu.CompilerParams(vmem_limit_bytes=67043328),
            name='insert_rows',
        )(seq_lens, hidden_out, k_new.reshape(layers, rows, kvh, hd), v_new.reshape(layers, rows, kvh, hd), k_suffix, v_suffix)
        return hidden_out, k_out, v_out

    return jax.shard_map(local_step, mesh=mesh, in_specs=(row_spec, lens_spec, whole_spec, whole_spec, whole_spec, whole_spec, prefix_spec, prefix_spec, cache_spec, cache_spec), out_specs=(row_spec, cache_spec, cache_spec), check_vma=False)
```

```python
import functools
import math

import jax
import jax.numpy as jnp
from jax import lax
from jax.experimental import pallas as pl
from jax.experimental.pallas import tpu as pltpu
from jax.sharding import PartitionSpec as P

MESH = pl.DeviceIdType.MESH
F32 = jnp.float32
BF16 = jnp.bfloat16
NEG = -1e30
UNROLL = 8
EARLY = 2
CHUNK = 1024
LOG2E = 1.4426950408889634


def decode_kernel(cfg, lens_ref, hid_ref, wq, wk, wv, wo, kp, vp, ks, vs,
                  out_ref, kn_ref, vn_ref,
                  wbuf, xbuf, qkv, qx, qall, raw, kf, kvsrc, kvbuf, sfx, sscr, mscr, osend, lsend, orecv, lrecv,
                  q3, n3, o3, l3, obuf,
                  w_sem, raw_sem, sfx_sem, x0_sem, q_ssem, q_rsem, qx_sem, kv_ssem, kv_rsem, kvm_rsem,
                  o_ssem, o_rsem, l_ssem, l_rsem, ob_sem, x_ssem, x_rsem):
    n_ctx, layers, rows, dim, kvh, grp, hd, pos, slots, nslot, ch = cfg
    chips = n_ctx // 2
    qw = grp * hd
    half_q = chips * qw
    half_kv = chips * hd
    xw = dim // (2 * chips)
    steps = 2 * chips + 2
    total = layers * steps
    scale = hd ** -0.5
    me = lax.axis_index('ctx')
    p = me // 2
    c = me % 2
    mate = 2 * p + (1 - c)
    far = chips // 2
    my_head = chips * c + p
    far_head = chips * c + (p + far) % chips
    near_len = 6 * pos
    my_rows = pl.ds(pl.multiple_of(c * rows, rows), rows)
    mate_rows = pl.ds(pl.multiple_of((1 - c) * rows, rows), rows)

    def issue_weights(g):
        lyr = g // steps
        j = g % steps
        slot = g % nslot

        @pl.when(g < total)
        def _():
            @pl.when(j < chips)
            def _():
                dest = (p + (j + chips // 2) % chips) % chips
                off = pl.multiple_of(c * half_q + dest * qw, 128)
                pltpu.make_async_copy(wq.at[lyr, :, pl.ds(off, qw)], wbuf.at[slot], w_sem.at[slot]).start()

            @pl.when(j == chips)
            def _():
                off = pl.multiple_of(c * half_kv, 128)
                pltpu.make_async_copy(wk.at[lyr, :, pl.ds(off, half_kv)], wbuf.at[slot], w_sem.at[slot]).start()

            @pl.when(j == chips + 1)
            def _():
                off = pl.multiple_of(c * half_kv, 128)
                pltpu.make_async_copy(wv.at[lyr, :, pl.ds(off, half_kv)], wbuf.at[slot], w_sem.at[slot]).start()

            @pl.when(j > chips + 1)
            def _():
                off = pl.multiple_of(c * (dim // 2) + (j - chips - 2) * xw, 128)
                pltpu.make_async_copy(wo.at[lyr, :, pl.ds(off, xw)], wbuf.at[slot], w_sem.at[slot]).start()

    def wait_weights(g):
        slot = g % nslot
        pltpu.make_async_copy(wq.at[0, :, pl.ds(0, qw)], wbuf.at[slot], w_sem.at[slot]).wait()
        return slot

    def raw_copies(lyr):
        return (pltpu.make_async_copy(kp.at[lyr], raw.at[0], raw_sem.at[0]),
                pltpu.make_async_copy(vp.at[lyr], raw.at[1], raw_sem.at[1]))

    def wait_kv_sent(slot, t):
        full = kvsrc.at[slot, t, pl.ds(0, 6)]
        pltpu.make_async_remote_copy(full, full, kv_ssem.at[slot, t], kv_rsem.at[0, 0],
                                     device_id={'ctx': mate}, device_id_type=MESH).wait_send()

    def prep_kv(lyr, t):
        slot = lyr % 2
        blk = 64
        pltpu.make_async_copy((kp, vp)[t].at[lyr], raw.at[t], raw_sem.at[t]).wait()

        def step(r, _):
            kf[...] = raw[t, pl.ds(pl.multiple_of(r * blk * kvh, 16), blk * kvh), :].astype(F32)
            for h in range(kvh):
                kvsrc[slot, t, h, pl.ds(pl.multiple_of(r * blk, blk), blk), :] = kf[pl.ds(h, blk, stride=kvh), :].astype(BF16)
            return 0
        lax.fori_loop(0, pos // blk, step, 0)
        kvbuf[lyr, t, pl.ds(pl.multiple_of(c * pos, pos), pos), :] = kvsrc[slot, t, my_head]
        kvbuf[lyr, t, pl.ds(pl.multiple_of((6 + c) * pos, pos), pos), :] = kvsrc[slot, t, far_head]

        @pl.when(lyr + 1 < layers)
        def _():
            pltpu.make_async_copy((kp, vp)[t].at[lyr + 1], raw.at[t], raw_sem.at[t]).start()

    def send_kv(lyr, t, head, place, dev, sem):
        slot = lyr % 2
        pltpu.make_async_remote_copy(
            kvsrc.at[slot, t, head], kvbuf.at[lyr, t, pl.ds(pl.multiple_of((place + c) * pos, pos), pos)],
            kv_ssem.at[slot, t], sem.at[lyr, t], device_id={'ctx': dev}, device_id_type=MESH).start()

    def send_kv_mate(lyr, t):
        send_kv(lyr, t, chips * (1 - c) + p, 0, mate, kvm_rsem)
        send_kv(lyr, t, chips * (1 - c) + (p + far) % chips, 6, mate, kvm_rsem)

    def send_kv_near(lyr, t, cc):
        up = (p + 1) % chips
        down = (p + chips - 1) % chips
        send_kv(lyr, t, chips * cc + up, 2, 2 * up + cc, kv_rsem)
        send_kv(lyr, t, chips * cc + down, 4, 2 * down + cc, kv_rsem)

    def wait_kv(lyr, t, sem, count):
        part = kvbuf.at[lyr, t, pl.ds(0, count * pos)]
        pltpu.make_async_remote_copy(part, part, kv_ssem.at[0, 0], sem.at[lyr, t],
                                     device_id={'ctx': mate}, device_id_type=MESH).wait_recv()

    def sfx_copies(lyr):
        return (pltpu.make_async_copy(ks.at[lyr], sfx.at[0], sfx_sem.at[0]),
                pltpu.make_async_copy(vs.at[lyr], sfx.at[1], sfx_sem.at[1]))

    own_x = pltpu.make_async_copy(hid_ref, xbuf.at[0, my_rows], x0_sem.at[2])
    own_x.start()
    for cp in raw_copies(0):
        cp.start()
    issue_weights(jnp.int32(0))
    barrier = pltpu.get_barrier_semaphore()
    for j in range(1, n_ctx):
        pl.semaphore_signal(barrier, inc=1, device_id={'ctx': (me + j) % n_ctx}, device_id_type=MESH)
    pl.semaphore_wait(barrier, n_ctx - 1)
    own_x.wait()
    x0 = pltpu.make_async_remote_copy(xbuf.at[0, my_rows], xbuf.at[0, my_rows], x0_sem.at[0], x0_sem.at[1],
                                      device_id={'ctx': mate}, device_id_type=MESH)
    x0.start()
    for t in range(2):
        prep_kv(jnp.int32(0), t)
        if t == 0:
            for g in range(1, nslot):
                issue_weights(jnp.int32(g))
            for cc in range(2):
                send_kv_near(jnp.int32(0), t, cc)
        send_kv_mate(jnp.int32(0), t)
    for cp in sfx_copies(0):
        cp.start()
    x0.wait()

    def q_copy(kind, head):
        dest = (head + far * kind) % chips
        return pltpu.make_async_remote_copy(qkv.at[head], qall.at[kind, p], q_ssem.at[kind, head], q_rsem.at[kind, p],
                                            device_id={'ctx': 2 * dest + c}, device_id_type=MESH)

    def q_recv(kind, src):
        return pltpu.make_async_remote_copy(qkv.at[src], qall.at[kind, src], q_ssem.at[kind, src], q_rsem.at[kind, src],
                                            device_id={'ctx': mate}, device_id_type=MESH)

    def o_copy(kind, dest, cc):
        to = (my_head, far_head)[kind]
        return pltpu.make_async_remote_copy(osend.at[kind, dest, cc], orecv.at[kind, to], o_ssem.at[kind, dest, cc], o_rsem.at[kind, to],
                                            device_id={'ctx': 2 * dest + cc}, device_id_type=MESH)

    def l_copy(kind, dest, cc):
        to = (my_head, far_head)[kind]
        return pltpu.make_async_remote_copy(lsend.at[kind, dest, cc], lrecv.at[kind, to], l_ssem.at[kind, dest, cc], l_rsem.at[kind, to],
                                            device_id={'ctx': 2 * dest + cc}, device_id_type=MESH)

    def layer(lyr, _):
        cur = lyr % 2
        nxt = 1 - cur
        base = lyr * steps

        def proj(t, _):
            g = base + t
            slot = wait_weights(g)
            val = jnp.dot(xbuf[cur], wbuf[slot], preferred_element_type=F32).astype(BF16)
            dest = jnp.where(t < chips, (p + (t + chips // 2) % chips) % chips, t)
            qkv[dest] = val

            @pl.when(t < chips)
            def _():
                for kind in range(2):
                    @pl.when((dest + far * kind) % chips != p)
                    def _():
                        q_copy(kind, dest).start()

                    @pl.when((dest + far * kind) % chips == p)
                    def _():
                        qall[kind, p] = val
            issue_weights(g + nslot)
            return 0

        lax.fori_loop(0, chips + 2, proj, 0)
        qx_cp = pltpu.make_async_remote_copy(qkv.at[:, mate_rows], qx, qx_sem.at[0], qx_sem.at[1],
                                             device_id={'ctx': mate}, device_id_type=MESH)
        qx_cp.start()

        @pl.when(lyr == 0)
        def _():
            for cc in range(2):
                send_kv_near(lyr, 1, cc)

        @pl.when((lyr == 0) & (layers > 1))
        def _():
            prep_kv(lyr + 1, 0)
            prep_kv(lyr + 1, 1)

        n_rows = 2 * grp * rows
        per = grp * rows
        rate = scale * LOG2E

        def src_at(kind, t):
            return (p + chips - t) % chips if kind else (p + t + 1) % chips

        def take_q(kind, t):
            src = src_at(kind, t)

            @pl.when(src != p)
            def _():
                q_recv(kind, src).wait_recv()
            return jnp.concatenate([qall[kind, src, cc * rows:(cc + 1) * rows, g * hd:(g + 1) * hd]
                                    for cc in range(2) for g in range(grp)], axis=0)

        def block(kind, lo, hi, t, score, value):
            old = mscr[...] if value else None
            qv = take_q(kind, t) if score else None
            if score:
                mx = jnp.full((n_rows, hd), NEG, F32)
            if value:
                acc = jnp.zeros((n_rows, hd), F32)
                ls = jnp.zeros((n_rows, hd), F32)
            for j in range(lo, hi, ch):
                if value:
                    e = jnp.exp2((sscr[:, j:j + ch] - old[:, 0:1]) * rate)
                if score:
                    s = lax.dot_general(qv, kvbuf[lyr, 0, j:j + ch, :], (((1,), (1,)), ((), ())), preferred_element_type=F32)
                    sscr[:, j:j + ch] = s
                if value:
                    for b in range(ch // hd):
                        ls = ls + e[:, b * hd:(b + 1) * hd]
                    acc = acc + jnp.dot(e.astype(BF16), kvbuf[lyr, 1, j:j + ch, :], preferred_element_type=F32)
                if score:
                    for b in range(ch // hd):
                        mx = jnp.maximum(mx, s[:, b * hd:(b + 1) * hd])
            if score:
                mscr[...] = jnp.broadcast_to(mx.max(axis=-1, keepdims=True), (n_rows, hd))
            if value:
                src = src_at(kind, t - 1)
                to = (my_head, far_head)[kind]
                mass = ls.sum(axis=-1, keepdims=True)
                o = (acc / mass).astype(BF16)
                lse = old * scale + jnp.log(mass)
                for cc in range(2):
                    dev = 2 * src + cc
                    for g in range(grp):
                        osend[kind, src, cc, :, g * hd:(g + 1) * hd] = o[cc * per + g * rows: cc * per + (g + 1) * rows]
                    lsend[kind, src, cc] = jnp.transpose(lse[cc * per:(cc + 1) * per])[0:8]

                    @pl.when(dev != me)
                    def _():
                        o_copy(kind, src, cc).start()
                        l_copy(kind, src, cc).start()

                    @pl.when(dev == me)
                    def _():
                        orecv[kind, to] = osend[kind, src, cc]
                        lrecv[kind, to] = lsend[kind, src, cc]

        def attention(kind, first, lo, hi):
            block(kind, lo, hi, first, True, False)

            def both(t, _):
                block(kind, lo, hi, t, True, True)
                return 0
            lax.fori_loop(first + 1, chips, both, 0)
            block(kind, lo, hi, chips, False, True)

        far_part = (near_len, near_len + 2 * pos)
        near_part = (0, near_len)
        wait_kv(lyr, 0, kvm_rsem, 2)
        wait_kv(lyr, 1, kvm_rsem, 2)
        block(1, *far_part, 0, True, False)
        block(1, *far_part, 1, False, True)

        qx_cp.wait_recv()
        mine = c * 1
        for h in range(kvh):
            own = mine == h // chips
            hh = h % chips
            for g in range(grp):
                sel = jnp.where(own, qkv[hh, my_rows, g * hd:(g + 1) * hd].astype(F32), qx[hh, :, g * hd:(g + 1) * hd].astype(F32))
                q3[pl.ds(h * grp + g, rows, stride=kvh * grp), :] = sel
            for t in range(2):
                sel = jnp.where(own, qkv[chips + t, my_rows, hh * hd:(hh + 1) * hd].astype(F32), qx[chips + t, :, hh * hd:(hh + 1) * hd].astype(F32))
                n3[t, pl.ds(h, rows, stride=kvh), :] = sel
        kn_ref[lyr] = n3[0].astype(BF16)
        vn_ref[lyr] = n3[1].astype(BF16)
        for cp in sfx_copies(lyr):
            cp.wait()
        nh = kvh * grp
        cols = slots * kvh
        l3[...] = jnp.zeros_like(l3)
        lane = lax.broadcasted_iota(jnp.int32, (nh, hd), 1)
        slot_id = lax.broadcasted_iota(jnp.int32, (slots, kvh, hd), 0)
        col_id = lax.broadcasted_iota(jnp.int32, (nh, cols), 1)
        row_id = lax.broadcasted_iota(jnp.int32, (nh, cols), 0)
        same = (col_id % kvh) == (row_id // grp)
        col_slot = jnp.where(same, col_id // kvh, slots + 1)
        unroll = UNROLL
        batches = rows // unroll
        early = jnp.where(lyr == 0, batches, EARLY)

        def suffix(i, _):
            bs = [i * unroll + u for u in range(unroll)]
            lns = [lens_ref[b] for b in bs]
            ats = [pl.ds(pl.multiple_of(b * nh, nh), nh) for b in bs]
            kv = []
            for b, ln in zip(bs, lns):
                hit = slot_id == ln
                for t in range(2):
                    new = n3[t, pl.ds(pl.multiple_of(b * kvh, kvh), kvh), :]
                    old = sfx[t, b].astype(F32).reshape(slots, kvh, hd)
                    kv.append(jnp.where(hit, new[None], old).reshape(cols, hd).astype(BF16))
            ss = [lax.dot_general(q3[at, :].astype(BF16), kv[2 * u], (((1,), (1,)), ((), ())), preferred_element_type=F32) * scale
                  for u, at in enumerate(ats)]
            ss = [jnp.where(col_slot <= ln, s, -jnp.inf) for s, ln in zip(ss, lns)]
            ms = [s.max(axis=-1, keepdims=True) for s in ss]
            es = [jnp.exp(s - m) for s, m in zip(ss, ms)]
            sums = [e.sum(axis=-1, keepdims=True) for e in es]
            os = [jnp.dot(e.astype(BF16), kv[2 * u + 1], preferred_element_type=F32) for u, e in enumerate(es)]
            for at, m, mass, o in zip(ats, ms, sums, os):
                o3[at, :] = o / mass
            part = l3[...]
            for b, m, mass in zip(bs, ms, sums):
                part = jnp.where(lane == b, m + jnp.log(mass), part)
            l3[...] = part
            return 0

        lax.fori_loop(0, early, suffix, 0)


        attention(1, 1, *far_part)
        wait_kv(lyr, 0, kv_rsem, 4)
        wait_kv(lyr, 1, kv_rsem, 4)
        attention(0, 0, *near_part)

        @pl.when(lyr + 1 < layers)
        def _():
            for t in range(2):
                for cc in range(2):
                    send_kv_near(lyr + 1, t, cc)
                send_kv_mate(lyr + 1, t)

        lax.fori_loop(early, batches, suffix, 0)

        @pl.when(lyr + 1 < layers)
        def _():
            for cp in sfx_copies(lyr + 1):
                cp.start()

        for kind in (1, 0):
            for h in range(kvh):
                @pl.when((my_head, far_head)[kind] != h)
                def _():
                    pltpu.make_async_remote_copy(osend.at[0, 0, 0], orecv.at[kind, h], o_ssem.at[0, 0, 0], o_rsem.at[kind, h],
                                                 device_id={'ctx': mate}, device_id_type=MESH).wait_recv()
                    pltpu.make_async_remote_copy(lsend.at[0, 0, 0], lrecv.at[kind, h], l_ssem.at[0, 0, 0], l_rsem.at[kind, h],
                                                 device_id={'ctx': mate}, device_id_type=MESH).wait_recv()
        parts = [jnp.concatenate([lrecv[kind, h, 0:1] for h in range(kvh)], axis=0) for kind in range(2)]
        own = l3[pl.ds(0, kvh, stride=grp), :]
        for g in range(1, grp):
            own = own + pltpu.roll(l3[pl.ds(g, kvh, stride=grp), :], g * rows, 1)
        parts.append(own)
        top = jnp.maximum(jnp.maximum(parts[0], parts[1]), parts[2])
        ups = [jnp.exp(x - top) for x in parts]
        inv = 1.0 / (ups[0] + ups[1] + ups[2])
        turn = jnp.transpose(jnp.concatenate([u * inv for u in ups] + [jnp.zeros((hd - 3 * kvh, hd), F32)], axis=0))
        for h in range(kvh):
            for g in range(grp):
                hx = h * grp + g
                wt = [turn[g * rows:(g + 1) * rows, i * kvh + h:i * kvh + h + 1] for i in range(3)]
                mix = (wt[0] * orecv[0, h, :, g * hd:(g + 1) * hd].astype(F32) + wt[1] * orecv[1, h, :, g * hd:(g + 1) * hd].astype(F32)
                       + wt[2] * o3[pl.ds(hx, rows, stride=kvh * grp), :])
                obuf[my_rows, hx * hd:(hx + 1) * hd] = mix.astype(BF16)
        ob = pltpu.make_async_remote_copy(obuf.at[my_rows], obuf.at[my_rows], ob_sem.at[0], ob_sem.at[1],
                                          device_id={'ctx': mate}, device_id_type=MESH)
        ob.start()

        def prep_ahead(t):
            @pl.when(lyr + 2 < layers)
            def _():
                wait_kv_sent(lyr % 2, t)
                prep_kv(lyr + 2, t)

        prep_ahead(0)
        ob.wait_recv()

        def x_copy(n):
            col = pl.ds(pl.multiple_of(c * (dim // 2) + n * xw, 128), xw)
            return pltpu.make_async_remote_copy(xbuf.at[nxt, :, col], xbuf.at[nxt, :, col], x_ssem.at[n], x_rsem.at[n],
                                                device_id={'ctx': mate}, device_id_type=MESH)

        def outp(n, _):
            g = base + chips + 2 + n
            slot = wait_weights(g)
            upd = jnp.dot(obuf[...], wbuf[slot], preferred_element_type=F32).astype(BF16)
            col = pl.ds(pl.multiple_of(c * (dim // 2) + n * xw, 128), xw)
            xbuf[nxt, :, col] = (xbuf[cur, :, col].astype(F32) + upd.astype(F32)).astype(BF16)
            x_copy(n).start()
            issue_weights(g + nslot)
            return 0

        lax.fori_loop(0, chips, outp, 0)
        prep_ahead(1)

        qx_cp.wait_send()
        ob.wait_send()
        for kind in range(2):
            for t in range(chips):
                @pl.when(p != (t + far * kind) % chips)
                def _():
                    q_copy(kind, t).wait_send()
                for cc in range(2):
                    @pl.when(me != 2 * t + cc)
                    def _():
                        o_copy(kind, t, cc).wait_send()
                        l_copy(kind, t, cc).wait_send()
        for n in range(chips):
            x_copy(n).wait()
        return 0

    lax.fori_loop(0, layers, layer, 0)
    for back in range(min(2, layers)):
        for t in range(2):
            wait_kv_sent((layers - 1 - back) % 2, t)
    out_ref[...] = xbuf[layers % 2, my_rows, :]


def insert_kernel(lens_ref, hid_ref, kn_ref, vn_ref, ks_ref, vs_ref, ho_ref, ko_ref, vo_ref,
                  hid, new, buf, h_sem, n_sem, in_sem, out_sem):
    layers, rows = ks_ref.shape[:2]
    sides = ((kn_ref, ks_ref, ko_ref), (vn_ref, vs_ref, vo_ref))
    news = [pltpu.make_async_copy(sides[t][0], new.at[t], n_sem.at[t]) for t in range(2)]
    loads = [(lyr, t, pltpu.make_async_copy(sides[t][1].at[lyr], buf.at[lyr, t], in_sem.at[lyr, t]))
             for lyr in range(layers) for t in range(2)]
    h_in = pltpu.make_async_copy(hid_ref, hid, h_sem.at[0])
    h_out = pltpu.make_async_copy(hid, ho_ref, h_sem.at[1])
    for cp in news:
        cp.start()
    for _, _, cp in loads:
        cp.start()
    h_in.start()
    for cp in news:
        cp.wait()
    stores = []
    for lyr, t, cp in loads:
        cp.wait()
        for b in range(rows):
            buf[lyr, t, b, lens_ref[b]] = new[t, lyr, b]
        out = pltpu.make_async_copy(buf.at[lyr, t], sides[t][2].at[lyr], out_sem.at[lyr, t])
        out.start()
        stores.append(out)
    h_in.wait()
    h_out.start()
    for out in stores:
        out.wait()
    h_out.wait()


def solution(mesh):
    n_ctx = mesh.shape['ctx']
    home_axes = ('data', 'ctx')
    row_spec = P(home_axes, None)
    lens_spec = P(home_axes)
    whole_spec = P()
    prefix_spec = P(None, home_axes, None, None)
    cache_spec = P(None, home_axes, None, None, None)

    def local_step(hidden, seq_lens, w_query, w_key, w_value, w_out, k_prefix, v_prefix, k_suffix, v_suffix):
        layers, pos, kvh, hd = k_prefix.shape
        rows, dim = hidden.shape
        slots = k_suffix.shape[2]
        grp = w_query.shape[2] // (kvh * hd)
        chips = n_ctx // 2
        qw = grp * hd
        nslot = 7
        ch = min(CHUNK, 2 * pos)
        cfg = (n_ctx, layers, rows, dim, kvh, grp, hd, pos, slots, nslot, ch)
        assert chips == 4 and kvh == n_ctx and chips * hd == qw and dim // n_ctx == qw and grp * rows == hd
        nh = kvh * grp
        vmem, anys, smem = pltpu.VMEM, pl.ANY, pltpu.SMEM
        hidden_out, k_new, v_new = pl.pallas_call(
            functools.partial(decode_kernel, cfg),
            out_shape=(jax.ShapeDtypeStruct((rows, dim), BF16),
                       jax.ShapeDtypeStruct((layers, rows * kvh, hd), BF16),
                       jax.ShapeDtypeStruct((layers, rows * kvh, hd), BF16)),
            in_specs=[pl.BlockSpec(memory_space=smem)] + [pl.BlockSpec(memory_space=anys)] * 9,
            out_specs=[pl.BlockSpec(memory_space=vmem)] * 3,
            scratch_shapes=[
                vmem((nslot, dim, qw), BF16),
                vmem((2, 2 * rows, dim), BF16),
                vmem((chips + 2, 2 * rows, qw), BF16),
                vmem((chips + 2, rows, qw), BF16),
                vmem((2, chips, 2 * rows, qw), BF16),
                vmem((2, pos * kvh, hd), BF16),
                vmem((64 * kvh, hd), F32),
                vmem((2, 2, kvh, pos, hd), BF16),
                vmem((layers, 2, n_ctx * pos, hd), BF16),
                vmem((2, rows, slots * kvh, hd), BF16),
                vmem((2 * grp * rows, n_ctx * pos), F32),
                vmem((2 * grp * rows, hd), F32),
                vmem((2, chips, 2, rows, qw), BF16),
                vmem((2, chips, 2, 8, hd), F32),
                vmem((2, kvh, rows, qw), BF16),
                vmem((2, kvh, 8, hd), F32),
                vmem((rows * nh, hd), F32),
                vmem((2, rows * kvh, hd), F32),
                vmem((rows * nh, hd), F32),
                vmem((nh, hd), F32),
                vmem((2 * rows, nh * hd), BF16),
                pltpu.SemaphoreType.DMA((nslot,)),
                pltpu.SemaphoreType.DMA((2,)),
                pltpu.SemaphoreType.DMA((2,)),
                pltpu.SemaphoreType.DMA((3,)),
                pltpu.SemaphoreType.DMA((2, chips)),
                pltpu.SemaphoreType.DMA((2, chips)),
                pltpu.SemaphoreType.DMA((2,)),
                pltpu.SemaphoreType.DMA((2, 2)),
                pltpu.SemaphoreType.DMA((layers, 2)),
                pltpu.SemaphoreType.DMA((layers, 2)),
                pltpu.SemaphoreType.DMA((2, chips, 2)),
                pltpu.SemaphoreType.DMA((2, kvh)),
                pltpu.SemaphoreType.DMA((2, chips, 2)),
                pltpu.SemaphoreType.DMA((2, kvh)),
                pltpu.SemaphoreType.DMA((2,)),
                pltpu.SemaphoreType.DMA((chips,)),
                pltpu.SemaphoreType.DMA((chips,)),
            ],
            compiler_params=pltpu.CompilerParams(collective_id=0, has_side_effects=True, vmem_limit_bytes=67043328),
            name='decode_layers',
        )(seq_lens, hidden, w_query, w_key, w_value, w_out,
          k_prefix.reshape(layers, pos * kvh, hd), v_prefix.reshape(layers, pos * kvh, hd),
          k_suffix.reshape(layers, rows, slots * kvh, hd), v_suffix.reshape(layers, rows, slots * kvh, hd))
        hidden_out, k_out, v_out = pl.pallas_call(
            insert_kernel,
            out_shape=(jax.ShapeDtypeStruct((rows, dim), BF16), jax.ShapeDtypeStruct(k_suffix.shape, BF16),
                       jax.ShapeDtypeStruct(v_suffix.shape, BF16)),
            in_specs=[pl.BlockSpec(memory_space=smem)] + [pl.BlockSpec(memory_space=anys)] * 5,
            out_specs=[pl.BlockSpec(memory_space=anys)] * 3,
            scratch_shapes=[
                vmem((rows, dim), BF16),
                vmem((2, layers, rows, kvh, hd), BF16),
                vmem((layers, 2, rows, slots, kvh, hd), BF16),
                pltpu.SemaphoreType.DMA((2,)),
                pltpu.SemaphoreType.DMA((2,)),
                pltpu.SemaphoreType.DMA((layers, 2)),
                pltpu.SemaphoreType.DMA((layers, 2)),
            ],
            compiler_params=pltpu.CompilerParams(vmem_limit_bytes=67043328),
            name='insert_rows',
        )(seq_lens, hidden_out, k_new.reshape(layers, rows, kvh, hd), v_new.reshape(layers, rows, kvh, hd), k_suffix, v_suffix)
        return hidden_out, k_out, v_out

    return jax.shard_map(local_step, mesh=mesh, in_specs=(row_spec, lens_spec, whole_spec, whole_spec, whole_spec, whole_spec, prefix_spec, prefix_spec, cache_spec, cache_spec), out_specs=(row_spec, cache_spec, cache_spec), check_vma=False)
```
